32 devices in a mesh: gx: 4 (over x, core), gy: 4 (over z), gz: 2 (over y).
Axes of the slice: x: 2, y: 2, z: 4, core: 2. Of those that a mesh axis runs over, the one named last changes fastest.
Arguments:
- attn_out: bfloat16 [704, 8192], P('gx', ('gz', 'gy')), may hold values from -6 to 6
- residual: bfloat16 [704, 8192], P('gx', ('gy', 'gz')), may hold values from -60 to 60
- proj_weight: bfloat16 [8192, 8192], P(('gz', 'gx'), 'gy'), may hold values from -0.0625 to 0.0625
- norm_gain: float32 [8192], P(('gy', 'gz')), may hold values from 0.1 to 1.9
- gate_proj: bfloat16 [8192, 14336], P(('gy', 'gx'), 'gz'), may hold values from -0.0625 to 0.0625
- up_proj: bfloat16 [8192, 14336], P(('gy', 'gx'), 'gz'), may hold values from -0.0625 to 0.0625
- down_proj: bfloat16 [14336, 8192], P(('gz', 'gx'), 'gy'), may hold values from -0.046875 to 0.046875
Outputs:
- layer_out: bfloat16 [704, 8192], P('gx', ('gy', 'gz'))
The draws below stay inside these ranges and needn't reach their ends.
All inputs are finite; a program needn't handle non-finite values.
Results may differ from the reference program's by a relative error of at most 0.0029.
Values may be sent and summed in bfloat16 or wider, within the bound.
A program may use at most 128 MiB of HBM per device.

```python
import jax
import jax.numpy as jnp
from jax import lax

D = 8192
FFW = 14336
TOKENS = 704


def draw_residual(key, part):
    first, second = jax.random.split(key, 2)
    ramp = 1.0 + 2.0 * jnp.arange(D, dtype=jnp.float32)[None, :] / (D - 1)
    values = jnp.clip(jax.random.normal(first, (TOKENS, D), jnp.float32), -6.0, 6.0)
    scales = jnp.exp(jax.random.uniform(second, (TOKENS, 1), jnp.float32, jnp.log(0.3), jnp.log(3.0)))
    return (values * scales * ramp).astype(jnp.bfloat16)


def block_scale(rng, shape, shards, smallest, high):
    loudness, own = 1.0, jax.random.fold_in(rng, 6)
    for dim, parts in shards:
        steps = jnp.exp(jax.random.uniform(jax.random.fold_in(own, dim), (parts,), jnp.float32, smallest / len(shards), high / len(shards)))
        loudness = loudness * jnp.repeat(steps, shape[dim] // parts).reshape([-1 if axis == dim else 1 for axis in range(len(shape))])
    return loudness


def centred(rng, extent, scale, reach, cuts=(), held_as=jnp.bfloat16):
    factor_of = block_scale(rng, extent, cuts, -0.22, 0.18) if cuts else 1.0
    result = jax.random.normal(rng, extent, jnp.float32) * scale * factor_of
    return jnp.minimum(jnp.maximum(result, -reach), reach).astype(held_as)


def setup_inputs(seed: int = 0) -> dict:
    key_of = jax.random.split(jax.random.key(seed), 8)
    return {
        "attn_out": centred(key_of[0], (TOKENS, D), 1.0, 6.0, ((0, 4), (1, 8))),
        "residual": draw_residual(jax.random.fold_in(key_of[7], 71), 0),
        "proj_weight": centred(key_of[2], (D, D), D ** -0.5, 0.0625, ((0, 8), (1, 4))),
        "norm_gain": jnp.clip(1.0 + 0.18 * jax.random.normal(key_of[3], (D,), jnp.float32), 0.1, 1.9),
        "gate_proj": centred(key_of[4], (D, FFW), D ** -0.5, 0.0625, ((0, 16), (1, 2))),
        "up_proj": centred(key_of[5], (D, FFW), D ** -0.5, 0.0625, ((0, 16), (1, 2))),
        "down_proj": centred(key_of[6], (FFW, D), FFW ** -0.5, 0.046875, ((0, 8), (1, 4))),
    }


def reference(attn_out, residual, proj_weight, norm_gain, gate_proj, up_proj, down_proj):
    projected = jnp.dot(attn_out, proj_weight, preferred_element_type=jnp.float32)
    stream = residual.astype(jnp.float32) + projected
    inverse = lax.rsqrt(lax.optimization_barrier(jnp.mean(stream * stream, axis=1, keepdims=True)) + 1e-05)
    scaled = (stream * norm_gain.astype(jnp.float32)[None, :]).astype(jnp.bfloat16)
    gate_sum = inverse * jnp.dot(scaled, gate_proj, preferred_element_type=jnp.float32)
    up_sum = inverse * jnp.dot(scaled, up_proj, preferred_element_type=jnp.float32)
    hidden = (jax.nn.silu(gate_sum) * up_sum).astype(jnp.bfloat16)
    down_sum = jnp.dot(hidden, down_proj, preferred_element_type=jnp.float32)
    return (stream + down_sum).astype(jnp.bfloat16)
```

```python
import functools

import jax
import jax.numpy as jnp
from jax import lax
from jax.experimental import pallas as pl
from jax.experimental.pallas import tpu as pltpu
from jax.sharding import PartitionSpec as P

LANES = 128
MESH = pl.DeviceIdType.MESH


def product(left, right):
    return jnp.dot(left, right, preferred_element_type=jnp.float32)


def swapped(value, axis, size, bit):
    return lax.ppermute(value, axis, [(i, i ^ bit) for i in range(size)])


def halved(blocks, axis, size, bit, rel=0):
    if bit == 1:
        return blocks(rel)
    bit //= 2
    away = halved(blocks, axis, size, bit, rel | bit).astype(jnp.bfloat16)
    return halved(blocks, axis, size, bit, rel) + swapped(away, axis, size, bit).astype(jnp.float32)


def reduced(blocks, axis, size):
    return halved(blocks, axis, size, size)


def pick(index, values):
    out = values[-1]
    for i in range(len(values) - 2, -1, -1):
        out = jnp.where(index == i, values[i], out)
    return out


def relay_order(n):
    return [sorted((d for d in range(n) if d != r), key=lambda d: (-abs(d - r), (d - r) * (1 if r >= n // 2 else -1)))
            for r in range(n)]


def ffn_kernel(
    n, chunk, width,
    scaled, stream, squares, gate, up, down, out,
    w, wd, lhs, relay, xs, xr, zr, hid, acc, tmp, inv, sqs,
    fs0, fr0, fsx, fsy, frx, fry, fsx2, fsy2, frx2, fry2,
    wl_sem, ws_sem, wr_sem, wd_sem, cs_sem, cr_sem, rr_sem, qs_sem, qr_sem,
    xs_sem, xr_sem, zs_sem, zr_sem, us_sem, ds_sem, hr_sem, fs_sem, fr_sem,
):
    x, r, y = lax.axis_index("gx"), lax.axis_index("gy"), lax.axis_index("gz")
    core, xc = x % 2, x // 2
    other = x + 1 - 2 * core
    across = (x + 2) % 4
    rows, home = scaled.shape
    depth = gate.shape[0]
    chunks = w.shape[1]
    hidden = chunks * chunk
    f32, bf16 = jnp.float32, jnp.bfloat16

    def at_x(i):
        return {"gx": i}

    def send(src, dst, ssem, rsem, where):
        return pltpu.make_async_remote_copy(
            src_ref=src, dst_ref=dst, send_sem=ssem, recv_sem=rsem,
            device_id=where, device_id_type=MESH)

    barrier = pltpu.get_barrier_semaphore()
    total = 4 * n * 2
    me = (x * n + r) * 2 + y

    def greet(i, carry):
        to = (me + i) % total
        pl.semaphore_signal(barrier, inc=1, device_id=(to // (2 * n), (to // 2) % n, to % 2), device_id_type=MESH)
        return carry

    lax.fori_loop(1, total, greet, 0)
    pl.semaphore_wait(barrier, total - 1)

    def columns(q, k, c):
        half = xc if q == 0 else 1 - xc
        return pl.ds(pl.multiple_of((2 * half + c) * hidden + k * chunk, LANES), chunk)

    mine = pl.ds(pl.multiple_of(core * depth, depth), depth)
    theirs = pl.ds(pl.multiple_of((1 - core) * depth, depth), depth)

    def fetch(k, carry):
        for q in (1, 0):
            for part, src in ((0, gate), (1, up)):
                lanes = pl.ds(part * chunk, chunk)
                pltpu.make_async_copy(
                    src.at[:, columns(q, k, core)], w.at[q, k, mine, lanes], wl_sem.at[q, k]).start()
                send(src.at[:, columns(q, k, 1 - core)], w.at[q, k, mine, lanes],
                     ws_sem.at[q, k], wr_sem.at[q, k], at_x(other)).start()
        return carry

    def await_weights(q, k):
        pltpu.make_async_copy(w.at[q, k, mine, :], w.at[q, k, mine, :], wl_sem.at[q, k]).wait()
        send(w.at[q, k, theirs, :], w.at[q, k, theirs, :], ws_sem.at[q, k], wr_sem.at[q, k], at_x(other)).wait_recv()

    same = xc == y
    y_other = {"gz": 1 - y}
    to_partner = send(scaled, lhs.at[x], cs_sem.at[0], cr_sem.at[x], at_x(other))
    to_y = send(scaled, lhs.at[x], cs_sem.at[1], cr_sem.at[x], y_other)
    to_x = send(scaled, lhs.at[x], cs_sem.at[0], cr_sem.at[x], at_x(across))
    to_relay = send(scaled, relay, cs_sem.at[1], rr_sem, y_other)
    from_relay = send(relay, lhs.at[x], cs_sem.at[2], cr_sem.at[x], at_x(across))
    pass_own = send(lhs.at[x], lhs.at[x], cs_sem.at[2], cr_sem.at[x], at_x(other))
    pass_across = send(lhs.at[across], lhs.at[across], cs_sem.at[3], cr_sem.at[across], at_x(other))

    @pl.when(same)
    def _():
        to_y.start()
        to_partner.start()
        lhs[x] = scaled[...]

    @pl.when(jnp.logical_not(same))
    def _():
        to_relay.start()
        to_x.start()

    slot = r * 2 + y

    def sq_copy(ox, oy):
        return send(squares, sqs.at[slot], qs_sem.at[ox, oy], qr_sem.at[slot],
                    ((x + ox) % 4, x, (y + oy) % 2))

    own_squares = r == x

    @pl.when(own_squares)
    def _():
        sqs[slot] = squares[...]

    @pl.when(jnp.logical_not(own_squares))
    def _():
        sq_copy(0, 0).start()

    for ox in range(4):
        for oy in range(2):
            if ox or oy:
                sq_copy(ox, oy).start()

    lax.fori_loop(0, chunks, fetch, 0)

    def fetch_down(k, carry):
        pltpu.make_async_copy(
            down.at[pl.ds(pl.multiple_of(k * chunk, chunk), chunk), :], wd.at[k], wd_sem.at[k]).start()
        return carry

    lax.fori_loop(0, chunks, fetch_down, 0)
    acc[...] = jnp.zeros_like(acc)

    @pl.when(same)
    def _():
        from_relay_in = send(relay, relay, cs_sem.at[1], rr_sem, y_other)
        from_relay_in.wait_recv()
        from_relay.start()

    @pl.when(jnp.logical_not(same))
    def _():
        pass_own.wait_recv()
        pass_own.start()

    pass_across.wait_recv()
    pass_across.start()
    third = (other + 2) % 4
    send(lhs.at[other], lhs.at[other], cs_sem.at[3], cr_sem.at[other], at_x(other)).wait_recv()
    send(lhs.at[third], lhs.at[third], cs_sem.at[3], cr_sem.at[third], at_x(other)).wait_recv()

    orders = relay_order(n)
    order = [pick(r, [orders[i][j] for i in range(n)]) for j in range(n - 1)]

    def send_chunk(k):
        await_weights(1, k)
        for d in order + [r]:
            xs[k, d] = product(lhs[d], w[1, k]).astype(bf16)
            send(xs.at[k, d], xr.at[k, d], xs_sem, xr_sem.at[k, d], at_x(across)).start()

    def own_term(k, d):
        send(xr.at[k, d], xr.at[k, d], xs_sem, xr_sem.at[k, d], at_x(across)).wait_recv()
        return product(lhs[d], w[0, k]) + xr[k, d].astype(f32)

    def z_copy(k, d):
        ahead = d > r
        nxt = jnp.where(ahead, r + 1, r - 1)
        place = jnp.where(jnp.logical_and(jnp.logical_not(ahead), d == r - 1), n, d)
        return send(xr.at[k, d], zr.at[k, place], zs_sem.at[k, d], zr_sem.at[k, place], {"gy": nxt})

    def z_wait(k, place):
        send(zr.at[k, place], zr.at[k, place], zs_sem.at[k, 0], zr_sem.at[k, place], {"gy": r}).wait_recv()

    def relay_chunk(k):
        await_weights(0, k)
        for d in order:
            tmp[...] = own_term(k, d)
            inner = jnp.logical_or(jnp.logical_and(d > r, r > 0), jnp.logical_and(d < r, r < n - 1))

            @pl.when(inner)
            def _():
                z_wait(k, d)
                tmp[...] = tmp[...] + zr[k, d].astype(f32)

            xr[k, d] = tmp[...].astype(bf16)
            z_copy(k, d).start()

    def up_copy(k, s):
        return send(hid.at[k, s], hid.at[k, s], us_sem.at[k, s], hr_sem.at[k, s], {"gy": r + 1})

    def down_copy(k, s):
        return send(hid.at[k, s], hid.at[k, s], ds_sem.at[k, s], hr_sem.at[k, s], {"gy": r - 1})

    def contract(k, s):
        acc[s] = acc[s] + product(hid[k, s], wd[k])

    def finish_chunk(k):
        tmp[...] = own_term(k, r)

        @pl.when(r > 0)
        def _():
            z_wait(k, r)
            tmp[...] = tmp[...] + zr[k, r].astype(f32)

        @pl.when(r < n - 1)
        def _():
            z_wait(k, n)
            tmp[...] = tmp[...] + zr[k, n].astype(f32)

        gate_sum = inv[...] * tmp[:, :chunk]
        up_sum = inv[...] * tmp[:, chunk:]
        hid[k, r] = (gate_sum / (1.0 + jnp.exp(-gate_sum)) * up_sum).astype(bf16)

        @pl.when(r < n - 1)
        def _():
            up_copy(k, r).start()

        @pl.when(r > 0)
        def _():
            down_copy(k, r).start()

        pltpu.make_async_copy(wd.at[k], wd.at[k], wd_sem.at[k]).wait()
        contract(k, r)

    def pass_chunk(k, step):
        @pl.when(r >= step)
        def _():
            up_copy(k, r - step).wait_recv()

            @pl.when(r < n - 1)
            def _():
                up_copy(k, r - step).start()

            contract(k, r - step)

        @pl.when(r + step < n)
        def _():
            down_copy(k, r + step).wait_recv()

            @pl.when(r > 0)
            def _():
                down_copy(k, r + step).start()

            contract(k, r + step)

    send_chunk(0)
    send_chunk(1)

    for i in range(2 * n):
        own = jnp.logical_and(x == r, slot == i)

        @pl.when(jnp.logical_not(own))
        def _():
            send(sqs.at[i], sqs.at[i], qs_sem.at[0, 0], qr_sem.at[i], {"gz": 1 - y}).wait_recv()

    summed = sqs[0]
    for i in range(1, 2 * n):
        summed = summed + sqs[i]
    inverse = lax.rsqrt(summed / width + 1e-05) * (1.0 / summed.shape[0])
    spread = lax.dot_general(
        inverse, jnp.ones((summed.shape[0], chunk), f32), (((0,), (0,)), ((), ())),
        precision=lax.Precision.HIGHEST, preferred_element_type=f32)
    inv[...] = spread[:rows]

    def body(t, carry):
        @pl.when(t + 2 < chunks)
        def _():
            send_chunk(t + 2)

        @pl.when(t < chunks)
        def _():
            relay_chunk(t)

        @pl.when(jnp.logical_and(t >= 1, t <= chunks))
        def _():
            finish_chunk(t - 1)

        for step in range(1, n):
            k = t - 1 - step

            @pl.when(jnp.logical_and(k >= 0, k < chunks))
            def _():
                pass_chunk(k, step)

        return carry

    lax.fori_loop(0, chunks + n, body, 0)

    half = home // 2
    for i in range(2):
        fs0[i] = acc[2 * i + 1 - core].astype(bf16)
    swap = send(fs0, fr0, fs_sem.at[0], fr_sem.at[0], at_x(other))
    swap.start()
    swap.wait_recv()

    def part(i, j, h):
        cols = pl.ds(pl.multiple_of(j * home + h * half, LANES), half)
        return acc[2 * i + core, :, cols] + fr0[i, :, cols].astype(f32)

    for i in range(2):
        fsx[i] = part(1 - xc, i, 0).astype(bf16)
    first_x = send(fsx, frx, fs_sem.at[1], fr_sem.at[1], at_x(across))
    first_x.start()
    for i in range(2):
        fsy[i] = part(i, 1 - y, 1).astype(bf16)
    first_y = send(fsy, fry, fs_sem.at[2], fr_sem.at[2], y_other)
    first_y.start()
    first_x.wait_recv()
    fsx2[...] = (part(xc, 1 - y, 0) + frx[1 - y].astype(f32)).astype(bf16)
    second_y = send(fsx2, frx2, fs_sem.at[3], fr_sem.at[3], y_other)
    second_y.start()
    first_y.wait_recv()
    fsy2[...] = (part(1 - xc, y, 1) + fry[1 - xc].astype(f32)).astype(bf16)
    second_x = send(fsy2, fry2, fs_sem.at[4], fr_sem.at[4], at_x(across))
    second_x.start()
    left = stream[:, :half] + part(xc, y, 0) + frx[y].astype(f32)
    right = stream[:, half:] + part(xc, y, 1) + fry[xc].astype(f32)
    second_y.wait_recv()
    out[:, :half] = (left + frx2[...].astype(f32)).astype(bf16)
    second_x.wait_recv()
    out[:, half:] = (right + fry2[...].astype(f32)).astype(bf16)

    for copy in (swap, first_x, first_y, second_y, second_x):
        copy.wait_send()
    send(xs, xs, xs_sem, xr_sem.at[0, 0], at_x(across)).wait_send()

    @pl.when(same)
    def _():
        to_y.wait_send()
        to_partner.wait_send()
        from_relay.wait_send()

    @pl.when(jnp.logical_not(same))
    def _():
        to_relay.wait_send()
        to_x.wait_send()
        pass_own.wait_send()

    pass_across.wait_send()

    @pl.when(jnp.logical_not(own_squares))
    def _():
        sq_copy(0, 0).wait_send()

    for ox in range(4):
        for oy in range(2):
            if ox or oy:
                sq_copy(ox, oy).wait_send()

    def drain(k, carry):
        for q in range(2):
            send(w.at[q, k, mine, :], w.at[q, k, mine, :], ws_sem.at[q, k], wr_sem.at[q, k], at_x(other)).wait_send()
        for d in order:
            z_copy(k, d).wait_send()

        @pl.when(r < n - 1)
        def _():
            up_copy(k, r).wait_send()

        @pl.when(r > 0)
        def _():
            down_copy(k, r).wait_send()

        for step in range(1, n):
            @pl.when(jnp.logical_and(r >= step, r < n - 1))
            def _():
                up_copy(k, r - step).wait_send()

            @pl.when(jnp.logical_and(r + step < n, r > 0))
            def _():
                down_copy(k, r + step).wait_send()

        return carry

    lax.fori_loop(0, chunks, drain, 0)


def ffn(sizes, scaled, stream, squares, gate_proj, up_proj, down_proj):
    gx, n, gz = sizes
    rows, home = scaled.shape
    depth = gate_proj.shape[0]
    hidden = gate_proj.shape[1] // gx
    width = home * n * gz
    chunk = 2 * LANES
    chunks = hidden // chunk
    cols = down_proj.shape[1]
    half = home // 2
    lanes = -(-rows // LANES) * LANES
    squares = jnp.broadcast_to(jnp.pad(squares, (0, lanes - rows))[None, :], (8, lanes))
    bf16, f32 = jnp.bfloat16, jnp.float32
    dma, vm = pltpu.SemaphoreType.DMA, pltpu.VMEM
    scratch = [
        vm((2, chunks, 2 * depth, 2 * chunk), bf16),
        vm((chunks, chunk, cols), bf16),
        vm((gx, rows, home), bf16),
        vm((rows, home), bf16),
        vm((chunks, n, rows, 2 * chunk), bf16),
        vm((chunks, n, rows, 2 * chunk), bf16),
        vm((chunks, n + 1, rows, 2 * chunk), bf16),
        vm((chunks, n, rows, chunk), bf16),
        vm((n, rows, cols), f32),
        vm((rows, 2 * chunk), f32),
        vm((rows, chunk), f32),
        vm((2 * n, 8, lanes), f32),
        vm((2, rows, cols), bf16), vm((2, rows, cols), bf16),
        vm((2, rows, half), bf16), vm((2, rows, half), bf16),
        vm((2, rows, half), bf16), vm((2, rows, half), bf16),
        vm((rows, half), bf16), vm((rows, half), bf16),
        vm((rows, half), bf16), vm((rows, half), bf16),
        dma((2, chunks)), dma((2, chunks)), dma((2, chunks)), dma((chunks,)),
        dma((4,)), dma((gx,)), dma, dma((gx, gz)), dma((2 * n,)),
        dma, dma((chunks, n)), dma((chunks, n)), dma((chunks, n + 1)),
        dma((chunks, n)), dma((chunks, n)), dma((chunks, n)), dma((5,)), dma((5,)),
    ]
    whole = pl.BlockSpec(memory_space=pltpu.VMEM)
    away = pl.BlockSpec(memory_space=pl.ANY)
    return pl.pallas_call(
        functools.partial(ffn_kernel, n, chunk, width),
        out_shape=jax.ShapeDtypeStruct((rows, home), bf16),
        in_specs=[whole] * 3 + [away] * 3,
        out_specs=whole,
        scratch_shapes=scratch,
        compiler_params=pltpu.CompilerParams(
            collective_id=0, has_side_effects=True, vmem_limit_bytes=67043328),
    )(scaled, stream, squares, gate_proj, up_proj, down_proj)


def on_device(sizes, attn_out, residual, proj_weight, norm_gain, gate_proj, up_proj, down_proj):
    gx, gy, gz = sizes
    assert gx == gy
    rows, home = residual.shape
    width = home * gy * gz
    x, z = lax.axis_index("gx"), lax.axis_index("gz")

    turn = [(i * gy + j, j * gy + i) for i in range(gx) for j in range(gy)]
    turned = lax.ppermute(attn_out, ("gx", "gy"), turn)
    cut = turned.shape[1] // 2
    attn_cols = [
        lax.all_gather(turned[:, at:at + cut], "gy", axis=0, tiled=True) for at in (0, cut)
    ]

    def scattered(lefts, weight):
        done, total = 0, None
        for left in lefts:
            depth = left.shape[1]
            part = product(left, lax.slice_in_dim(weight, done, done + depth, axis=0))
            done += depth
            total = part if total is None else total + part

        def columns(zrel):
            def term(xrel):
                at = ((x ^ xrel) * rows, (z ^ zrel) * home)
                return lax.dynamic_slice(total, at, (rows, home))
            return reduced(term, "gx", gx)
        return reduced(columns, "gz", gz)

    projected = scattered(attn_cols, proj_weight)
    stream = residual.astype(jnp.float32) + projected
    scaled = (stream * norm_gain[None, :]).astype(jnp.bfloat16)
    squares = jnp.sum(stream * stream, axis=1)
    if gx == 4 and gz == 2:
        return ffn(sizes, scaled, stream, squares, gate_proj, up_proj, down_proj)

    scaled = lax.all_gather(scaled, "gz", axis=1, tiled=True)
    scaled = lax.all_to_all(scaled, "gx", split_axis=1, concat_axis=0, tiled=True)
    for axis, size in (("gy", gy), ("gz", gz)):
        bit = 1
        while bit < size:
            squares = squares + swapped(squares, axis, size, bit)
            bit *= 2
    squares = lax.ppermute(squares, ("gx", "gy"), turn)
    inverse = lax.rsqrt(squares / width + 1e-05)[:, None]

    block = gate_proj.shape[1] // gx
    head = 3 * block // 7
    top = gx // 2

    def term_of(weight, at, size, left):
        def term(rel):
            return product(
                left, lax.dynamic_slice_in_dim(weight, (x ^ rel) * block + at, size, 1)
            )
        return term

    def far(at, size, left):
        return [
            halved(term_of(weight, at, size, left), "gx", gx, top, top).astype(jnp.bfloat16)
            for weight in (gate_proj, up_proj)
        ]

    def joined(at, size, left, arrived):
        parts = [
            (halved(term_of(weight, at, size, left), "gx", gx, top) + part.astype(jnp.float32))
            for weight, part in zip((gate_proj, up_proj), arrived)
        ]
        return jnp.concatenate([part.astype(jnp.bfloat16) for part in parts], axis=1)

    def activated(both):
        both = lax.psum_scatter(both, "gy", scatter_dimension=0, tiled=True).astype(jnp.float32)
        half = both.shape[1] // 2
        gate_sum, up_sum = inverse * both[:, :half], inverse * both[:, half:]
        piece = (jax.nn.silu(gate_sum) * up_sum).astype(jnp.bfloat16)
        return lax.all_gather(piece, "gy", axis=0, tiled=True)

    first = [swapped(part, "gx", gx, top) for part in far(0, head, scaled)]
    second = far(head, block - head, scaled)
    first, second = lax.optimization_barrier((first, second))
    second = [swapped(part, "gx", gx, top) for part in second]
    early = activated(joined(0, head, scaled, first))
    late = joined(head, block - head, scaled, second)
    early, late = lax.optimization_barrier((early, late))
    hidden = [early, activated(late)]

    down_sum = scattered(hidden, down_proj)
    return (stream + down_sum).astype(jnp.bfloat16)


def solution(mesh):
    sizes = tuple(mesh.shape[name] for name in ("gx", "gy", "gz"))
    in_specs = (
        P("gx", ("gz", "gy")),
        P("gx", ("gy", "gz")),
        P(("gz", "gx"), "gy"),
        P(("gy", "gz")),
        P(("gy", "gx"), "gz"),
        P(("gy", "gx"), "gz"),
        P(("gz", "gx"), "gy"),
    )
    out_specs = P("gx", ("gy", "gz"))
    return jax.shard_map(
        lambda *args: on_device(sizes, *args),
        mesh=mesh, in_specs=in_specs, out_specs=out_specs, check_vma=False,
    )
```

```python
import functools

import jax
import jax.numpy as jnp
from jax import lax
from jax.experimental import pallas as pl
from jax.experimental.pallas import tpu as pltpu
from jax.sharding import PartitionSpec as P

LANES = 128
MESH = pl.DeviceIdType.MESH


def product(left, right):
    return jnp.dot(left, right, preferred_element_type=jnp.float32)


def swapped(value, axis, size, bit):
    return lax.ppermute(value, axis, [(i, i ^ bit) for i in range(size)])


def halved(blocks, axis, size, bit, rel=0):
    if bit == 1:
        return blocks(rel)
    bit //= 2
    away = halved(blocks, axis, size, bit, rel | bit).astype(jnp.bfloat16)
    return halved(blocks, axis, size, bit, rel) + swapped(away, axis, size, bit).astype(jnp.float32)


def reduced(blocks, axis, size):
    return halved(blocks, axis, size, size)


def pick(index, values):
    out = values[-1]
    for i in range(len(values) - 2, -1, -1):
        out = jnp.where(index == i, values[i], out)
    return out


def relay_order(n):
    return [sorted((d for d in range(n) if d != r), key=lambda d: (-abs(d - r), (d - r) * (1 if r >= n // 2 else -1)))
            for r in range(n)]


def layer_kernel(
    n, chunk, width,
    attn, residual, gain, proj, gate, up, down, out,
    w, wd, att, atx, res, stream, scaled, gains, lhs, relay, xs, xr, zr, hid, acc, tmp, inv, sq, sqs,
    fs0, fr0, fsx, fsy, frx, fry, fsx2, fsy2, frx2, fry2,
    wl_sem, ws_sem, wr_sem, wd_sem, pl_sem, ps_sem, pr_sem, io_sem,
    al_sem, au_sem, ad_sem, ar_sem, ax_sem, axr_sem,
    cs_sem, cr_sem, rr_sem, qs_sem, qr_sem,
    xs_sem, xr_sem, zs_sem, zr_sem, us_sem, ds_sem, hr_sem, fs_sem, fr_sem,
):
    x, r, y = lax.axis_index("gx"), lax.axis_index("gy"), lax.axis_index("gz")
    core, xc = x % 2, x // 2
    other = x + 1 - 2 * core
    across = (x + 2) % 4
    rows, home = stream.shape
    half = home // 2
    depth = gate.shape[0]
    chunks = w.shape[1]
    hidden = chunks * chunk
    f32, bf16 = jnp.float32, jnp.bfloat16

    def at_x(i):
        return {"gx": i}

    y_other = {"gz": 1 - y}

    def send(src, dst, ssem, rsem, where):
        return pltpu.make_async_remote_copy(
            src_ref=src, dst_ref=dst, send_sem=ssem, recv_sem=rsem,
            device_id=where, device_id_type=MESH)

    def side(h):
        return pl.ds(h * half, half)

    own_proj = pl.ds(pl.multiple_of(core * home, home), home)
    for h in range(2):
        pltpu.make_async_copy(attn.at[:, side(h)], att.at[r, h], al_sem.at[h]).start()
    proj_in = pltpu.make_async_copy(proj, wd.at[own_proj, :], pl_sem)
    proj_in.start()
    res_in = pltpu.make_async_copy(residual, res, io_sem.at[0])
    res_in.start()
    gain_in = pltpu.make_async_copy(gain, gains, io_sem.at[1])
    gain_in.start()

    barrier = pltpu.get_barrier_semaphore()
    total = 4 * n * 2
    me = (x * n + r) * 2 + y

    def greet(i, carry):
        to = (me + i) % total
        pl.semaphore_signal(barrier, inc=1, device_id=(to // (2 * n), (to // 2) % n, to % 2), device_id_type=MESH)
        return carry

    lax.fori_loop(1, total, greet, 0)
    pl.semaphore_wait(barrier, total - 1)

    def a_up(s, h):
        return send(att.at[s, h], att.at[s, h], au_sem.at[s, h], ar_sem.at[s, h], {"gy": r + 1})

    def a_down(s, h):
        return send(att.at[s, h], att.at[s, h], ad_sem.at[s, h], ar_sem.at[s, h], {"gy": r - 1})

    def a_x(s, h):
        return send(att.at[s, h], atx.at[s % 2, h], ax_sem.at[s, h], axr_sem.at[s % 2, h], at_x(across))

    for h in range(2):
        pltpu.make_async_copy(attn.at[:, side(h)], att.at[r, h], al_sem.at[h]).wait()

        @pl.when(r < n - 1)
        def _():
            a_up(r, h).start()

        @pl.when(r > 0)
        def _():
            a_down(r, h).start()

        @pl.when(r // 2 != xc)
        def _():
            a_x(r, h).start()

    proj_out = send(proj, wd.at[own_proj, :], ps_sem, pr_sem, at_x(other))
    proj_out.start()

    def columns(q, k, c):
        place = xc if q == 0 else 1 - xc
        return pl.ds(pl.multiple_of((2 * place + c) * hidden + k * chunk, LANES), chunk)

    mine = pl.ds(pl.multiple_of(core * depth, depth), depth)
    theirs = pl.ds(pl.multiple_of((1 - core) * depth, depth), depth)

    def fetch(k, carry):
        for q in (1, 0):
            for part, src in ((0, gate), (1, up)):
                lanes = pl.ds(part * chunk, chunk)
                pltpu.make_async_copy(
                    src.at[:, columns(q, k, core)], w.at[q, k, mine, lanes], wl_sem.at[q, k]).start()
                send(src.at[:, columns(q, k, 1 - core)], w.at[q, k, mine, lanes],
                     ws_sem.at[q, k], wr_sem.at[q, k], at_x(other)).start()
        return carry

    def await_weights(q, k):
        pltpu.make_async_copy(w.at[q, k, mine, :], w.at[q, k, mine, :], wl_sem.at[q, k]).wait()
        send(w.at[q, k, theirs, :], w.at[q, k, theirs, :], ws_sem.at[q, k], wr_sem.at[q, k], at_x(other)).wait_recv()

    lax.fori_loop(0, chunks, fetch, 0)

    for step in range(1, n):
        for h in range(2):
            @pl.when(r >= step)
            def _():
                s = r - step
                a_up(s, h).wait_recv()

                @pl.when(r < n - 1)
                def _():
                    a_up(s, h).start()

                @pl.when(s // 2 != xc)
                def _():
                    a_x(s, h).start()

            @pl.when(r + step < n)
            def _():
                s = r + step
                a_down(s, h).wait_recv()

                @pl.when(r > 0)
                def _():
                    a_down(s, h).start()

                @pl.when(s // 2 != xc)
                def _():
                    a_x(s, h).start()

    proj_in.wait()
    proj_out.wait_recv()
    tile = 2 * chunk

    def project(rows_of, to):
        def body(j, carry):
            cols = pl.ds(pl.multiple_of(j * tile, tile), tile)
            value = None
            for i in range(2):
                for h in range(2):
                    term = product(rows_of(i, h), wd[i * home + h * half:i * home + (h + 1) * half, cols])
                    value = term if value is None else value + term
            acc[to, :, cols] = value
            return carry

        lax.fori_loop(0, acc.shape[2] // tile, body, 0)

    project(lambda i, h: att[2 * xc + i, h], xc)
    for h in range(2):
        for i in range(2):
            send(atx.at[i, h], atx.at[i, h], ax_sem.at[0, h], axr_sem.at[i, h], at_x(across)).wait_recv()
    project(lambda i, h: atx[i, h], 1 - xc)

    def copies():
        return (
            send(fsx, frx, fs_sem.at[1], fr_sem.at[1], at_x(across)),
            send(fsy, fry, fs_sem.at[2], fr_sem.at[2], y_other),
            send(fsx2, frx2, fs_sem.at[3], fr_sem.at[3], y_other),
            send(fsy2, fry2, fs_sem.at[4], fr_sem.at[4], at_x(across)),
        )

    def reduce_xy(part, finish):
        first_x, first_y, second_y, second_x = copies()
        for j in range(2):
            fsx[j] = part(1 - xc, j, 0).astype(bf16)
        first_x.start()
        for i in range(2):
            fsy[i] = part(i, 1 - y, 1).astype(bf16)
        first_y.start()
        first_x.wait_recv()
        fsx2[...] = (part(xc, 1 - y, 0) + frx[1 - y].astype(f32)).astype(bf16)
        second_y.start()
        first_y.wait_recv()
        fsy2[...] = (part(1 - xc, y, 1) + fry[1 - xc].astype(f32)).astype(bf16)
        second_x.start()
        second_y.wait_recv()
        finish(0, part(xc, y, 0) + frx[y].astype(f32) + frx2[...].astype(f32))
        second_x.wait_recv()
        finish(1, part(xc, y, 1) + fry[xc].astype(f32) + fry2[...].astype(f32))
        for copy in (first_x, first_y, second_y, second_x):
            copy.wait_send()

    same = xc == y

    def lanes_of(ref, slot, h):
        return ref.at[slot, :, side(h)]

    def to_partner(h):
        return send(scaled.at[h], lanes_of(lhs, x, h), cs_sem.at[0, h], cr_sem.at[x, h], at_x(other))

    def to_y(h):
        return send(scaled.at[h], lanes_of(lhs, x, h), cs_sem.at[1, h], cr_sem.at[x, h], y_other)

    def to_x(h):
        return send(scaled.at[h], lanes_of(lhs, x, h), cs_sem.at[0, h], cr_sem.at[x, h], at_x(across))

    def to_relay(h):
        return send(scaled.at[h], relay.at[h], cs_sem.at[1, h], rr_sem.at[h], y_other)

    def from_relay(h):
        return send(relay.at[h], lanes_of(lhs, x, h), cs_sem.at[2, h], cr_sem.at[x, h], at_x(across))

    def pass_own(h):
        return send(lanes_of(lhs, x, h), lanes_of(lhs, x, h), cs_sem.at[2, h], cr_sem.at[x, h], at_x(other))

    def pass_across(h):
        return send(lanes_of(lhs, across, h), lanes_of(lhs, across, h), cs_sem.at[3, h], cr_sem.at[across, h], at_x(other))

    def arrived(slot, h):
        send(lanes_of(lhs, slot, h), lanes_of(lhs, slot, h), cs_sem.at[3, h], cr_sem.at[slot, h], at_x(other)).wait_recv()

    def project_part(i, j, h):
        return acc[i, :, pl.ds(pl.multiple_of(j * home + h * half, LANES), half)]

    res_in.wait()
    gain_in.wait()

    def streamed(h, value):
        value = value + res[:, h * half:(h + 1) * half].astype(f32)
        stream[:, h * half:(h + 1) * half] = value
        value = (value * gains[:, h * half:(h + 1) * half]).astype(bf16)
        scaled[h] = value

        @pl.when(same)
        def _():
            to_y(h).start()
            to_partner(h).start()
            lhs[x, :, side(h)] = value

        @pl.when(jnp.logical_not(same))
        def _():
            to_relay(h).start()
            to_x(h).start()

    reduce_xy(project_part, streamed)

    slot = r * 2 + y

    def sq_copy(ox, oy):
        return send(sq, sqs.at[slot], qs_sem.at[ox, oy], qr_sem.at[slot],
                    ((x + ox) % 4, x, (y + oy) % 2))

    own_squares = r == x
    sq[...] = jnp.zeros_like(sq)
    squares = stream[...] * stream[...]
    sq[:, :rows] = lax.dot_general(
        jnp.ones((sq.shape[0], home), f32), squares, (((1,), (1,)), ((), ())),
        precision=lax.Precision.HIGHEST, preferred_element_type=f32)

    @pl.when(own_squares)
    def _():
        sqs[slot] = sq[...]

    @pl.when(jnp.logical_not(own_squares))
    def _():
        sq_copy(0, 0).start()

    for ox in range(4):
        for oy in range(2):
            if ox or oy:
                sq_copy(ox, oy).start()

    def fetch_down(k, carry):
        place = pl.ds(pl.multiple_of(k * chunk, chunk), chunk)
        pltpu.make_async_copy(down.at[place, :], wd.at[place, :], wd_sem.at[k]).start()
        return carry

    lax.fori_loop(0, chunks, fetch_down, 0)
    acc[...] = jnp.zeros_like(acc)

    for h in range(2):
        @pl.when(same)
        def _():
            send(relay.at[h], relay.at[h], cs_sem.at[1, h], rr_sem.at[h], y_other).wait_recv()
            from_relay(h).start()

        @pl.when(jnp.logical_not(same))
        def _():
            arrived(x, h)
            pass_own(h).start()

        arrived(across, h)
        pass_across(h).start()

    third = (other + 2) % 4
    for h in range(2):
        arrived(other, h)
        arrived(third, h)

    orders = relay_order(n)
    order = [pick(r, [orders[i][j] for i in range(n)]) for j in range(n - 1)]

    def send_chunk(k):
        await_weights(1, k)
        for d in order + [r]:
            xs[k, d] = product(lhs[d], w[1, k]).astype(bf16)
            send(xs.at[k, d], xr.at[k, d], xs_sem, xr_sem.at[k, d], at_x(across)).start()

    def own_term(k, d):
        send(xr.at[k, d], xr.at[k, d], xs_sem, xr_sem.at[k, d], at_x(across)).wait_recv()
        return product(lhs[d], w[0, k]) + xr[k, d].astype(f32)

    def z_copy(k, d):
        ahead = d > r
        nxt = jnp.where(ahead, r + 1, r - 1)
        place = jnp.where(jnp.logical_and(jnp.logical_not(ahead), d == r - 1), n, d)
        return send(xr.at[k, d], zr.at[k, place], zs_sem.at[k, d], zr_sem.at[k, place], {"gy": nxt})

    def z_wait(k, place):
        send(zr.at[k, place], zr.at[k, place], zs_sem.at[k, 0], zr_sem.at[k, place], {"gy": r}).wait_recv()

    def relay_chunk(k):
        await_weights(0, k)
        for d in order:
            tmp[...] = own_term(k, d)
            inner = jnp.logical_or(jnp.logical_and(d > r, r > 0), jnp.logical_and(d < r, r < n - 1))

            @pl.when(inner)
            def _():
                z_wait(k, d)
                tmp[...] = tmp[...] + zr[k, d].astype(f32)

            xr[k, d] = tmp[...].astype(bf16)
            z_copy(k, d).start()

    def up_copy(k, s):
        return send(hid.at[k, s], hid.at[k, s], us_sem.at[k, s], hr_sem.at[k, s], {"gy": r + 1})

    def down_copy(k, s):
        return send(hid.at[k, s], hid.at[k, s], ds_sem.at[k, s], hr_sem.at[k, s], {"gy": r - 1})

    def down_rows(k):
        return pl.ds(pl.multiple_of(k * chunk, chunk), chunk)

    def contract(k, s):
        acc[s] = acc[s] + product(hid[k, s], wd[down_rows(k), :])

    def finish_chunk(k):
        tmp[...] = own_term(k, r)

        @pl.when(r > 0)
        def _():
            z_wait(k, r)
            tmp[...] = tmp[...] + zr[k, r].astype(f32)

        @pl.when(r < n - 1)
        def _():
            z_wait(k, n)
            tmp[...] = tmp[...] + zr[k, n].astype(f32)

        gate_sum = inv[...] * tmp[:, :chunk]
        up_sum = inv[...] * tmp[:, chunk:]
        hid[k, r] = (gate_sum / (1.0 + jnp.exp(-gate_sum)) * up_sum).astype(bf16)

        @pl.when(r < n - 1)
        def _():
            up_copy(k, r).start()

        @pl.when(r > 0)
        def _():
            down_copy(k, r).start()

        pltpu.make_async_copy(wd.at[down_rows(k), :], wd.at[down_rows(k), :], wd_sem.at[k]).wait()
        contract(k, r)

    def pass_chunk(k, step):
        @pl.when(r >= step)
        def _():
            up_copy(k, r - step).wait_recv()

            @pl.when(r < n - 1)
            def _():
                up_copy(k, r - step).start()

            contract(k, r - step)

        @pl.when(r + step < n)
        def _():
            down_copy(k, r + step).wait_recv()

            @pl.when(r > 0)
            def _():
                down_copy(k, r + step).start()

            contract(k, r + step)

    send_chunk(0)
    send_chunk(1)

    for i in range(2 * n):
        own = jnp.logical_and(x == r, slot == i)

        @pl.when(jnp.logical_not(own))
        def _():
            send(sqs.at[i], sqs.at[i], qs_sem.at[0, 0], qr_sem.at[i], y_other).wait_recv()

    summed = sqs[0]
    for i in range(1, 2 * n):
        summed = summed + sqs[i]
    inverse = lax.rsqrt(summed / width + 1e-05) * (1.0 / summed.shape[0])
    spread = lax.dot_general(
        inverse, jnp.ones((summed.shape[0], chunk), f32), (((0,), (0,)), ((), ())),
        precision=lax.Precision.HIGHEST, preferred_element_type=f32)
    inv[...] = spread[:rows]

    def body(t, carry):
        @pl.when(t + 2 < chunks)
        def _():
            send_chunk(t + 2)

        @pl.when(t < chunks)
        def _():
            relay_chunk(t)

        @pl.when(jnp.logical_and(t >= 1, t <= chunks))
        def _():
            finish_chunk(t - 1)

        for step in range(1, n):
            k = t - 1 - step

            @pl.when(jnp.logical_and(k >= 0, k < chunks))
            def _():
                pass_chunk(k, step)

        return carry

    lax.fori_loop(0, chunks + n, body, 0)

    for i in range(2):
        fs0[i] = acc[2 * i + 1 - core].astype(bf16)
    swap = send(fs0, fr0, fs_sem.at[0], fr_sem.at[0], at_x(other))
    swap.start()
    swap.wait_recv()

    def down_part(i, j, h):
        cols = pl.ds(pl.multiple_of(j * home + h * half, LANES), half)
        return acc[2 * i + core, :, cols] + fr0[i, :, cols].astype(f32)

    def written(h, value):
        out[:, h * half:(h + 1) * half] = (stream[:, h * half:(h + 1) * half] + value).astype(bf16)

    reduce_xy(down_part, written)

    swap.wait_send()
    proj_out.wait_send()
    send(xs, xs, xs_sem, xr_sem.at[0, 0], at_x(across)).wait_send()

    for h in range(2):
        @pl.when(same)
        def _():
            to_y(h).wait_send()
            to_partner(h).wait_send()
            from_relay(h).wait_send()

        @pl.when(jnp.logical_not(same))
        def _():
            to_relay(h).wait_send()
            to_x(h).wait_send()
            pass_own(h).wait_send()

        pass_across(h).wait_send()

        for s in range(n):
            @pl.when(jnp.logical_and(s <= r, r < n - 1))
            def _():
                a_up(s, h).wait_send()

            @pl.when(jnp.logical_and(s >= r, r > 0))
            def _():
                a_down(s, h).wait_send()

            @pl.when(s // 2 != xc)
            def _():
                a_x(s, h).wait_send()

    @pl.when(jnp.logical_not(own_squares))
    def _():
        sq_copy(0, 0).wait_send()

    for ox in range(4):
        for oy in range(2):
            if ox or oy:
                sq_copy(ox, oy).wait_send()

    def drain(k, carry):
        for q in range(2):
            send(w.at[q, k, mine, :], w.at[q, k, mine, :], ws_sem.at[q, k], wr_sem.at[q, k], at_x(other)).wait_send()
        for d in order:
            z_copy(k, d).wait_send()

        for s in range(n):
            @pl.when(jnp.logical_and(s <= r, r < n - 1))
            def _():
                up_copy(k, s).wait_send()

            @pl.when(jnp.logical_and(s >= r, r > 0))
            def _():
                down_copy(k, s).wait_send()

        return carry

    lax.fori_loop(0, chunks, drain, 0)


def layer(sizes, attn_out, residual, proj_weight, norm_gain, gate_proj, up_proj, down_proj):
    gx, n, gz = sizes
    rows, home = residual.shape
    depth = gate_proj.shape[0]
    hidden = gate_proj.shape[1] // gx
    width = home * n * gz
    chunk = 2 * LANES
    chunks = hidden // chunk
    cols = down_proj.shape[1]
    half = home // 2
    lanes = -(-rows // LANES) * LANES
    bf16, f32 = jnp.bfloat16, jnp.float32
    dma, vm = pltpu.SemaphoreType.DMA, pltpu.VMEM
    scratch = [
        vm((2, chunks, 2 * depth, 2 * chunk), bf16),
        vm((max(2 * home, hidden), cols), bf16),
        vm((n, 2, rows, half), bf16),
        vm((2, 2, rows, half), bf16),
        vm((rows, home), bf16),
        vm((rows, home), f32),
        vm((2, rows, half), bf16),
        vm((1, home), f32),
        vm((gx, rows, home), bf16),
        vm((2, rows, half), bf16),
        vm((chunks, n, rows, 2 * chunk), bf16),
        vm((chunks, n, rows, 2 * chunk), bf16),
        vm((chunks, n + 1, rows, 2 * chunk), bf16),
        vm((chunks, n, rows, chunk), bf16),
        vm((n, rows, cols), f32),
        vm((rows, 2 * chunk), f32),
        vm((rows, chunk), f32),
        vm((8, lanes), f32),
        vm((2 * n, 8, lanes), f32),
        vm((2, rows, cols), bf16), vm((2, rows, cols), bf16),
        vm((2, rows, half), bf16), vm((2, rows, half), bf16),
        vm((2, rows, half), bf16), vm((2, rows, half), bf16),
        vm((rows, half), bf16), vm((rows, half), bf16),
        vm((rows, half), bf16), vm((rows, half), bf16),
        dma((2, chunks)), dma((2, chunks)), dma((2, chunks)), dma((chunks,)),
        dma, dma, dma, dma((2,)),
        dma((2,)), dma((n, 2)), dma((n, 2)), dma((n, 2)), dma((n, 2)), dma((2, 2)),
        dma((4, 2)), dma((gx, 2)), dma((2,)), dma((gx, gz)), dma((2 * n,)),
        dma, dma((chunks, n)), dma((chunks, n)), dma((chunks, n + 1)),
        dma((chunks, n)), dma((chunks, n)), dma((chunks, n)), dma((5,)), dma((5,)),
    ]
    away = pl.BlockSpec(memory_space=pl.ANY)
    return pl.pallas_call(
        functools.partial(layer_kernel, n, chunk, width),
        out_shape=jax.ShapeDtypeStruct((rows, home), bf16),
        in_specs=[away] * 7,
        out_specs=pl.BlockSpec(memory_space=pltpu.VMEM),
        scratch_shapes=scratch,
        compiler_params=pltpu.CompilerParams(
            collective_id=0, has_side_effects=True, vmem_limit_bytes=67043328),
    )(attn_out, residual, norm_gain[None, :], proj_weight, gate_proj, up_proj, down_proj)


def on_device(sizes, attn_out, residual, proj_weight, norm_gain, gate_proj, up_proj, down_proj):
    gx, gy, gz = sizes
    assert gx == gy
    if gx == 4 and gz == 2:
        return layer(sizes, attn_out, residual, proj_weight, norm_gain, gate_proj, up_proj, down_proj)
    rows, home = residual.shape
    width = home * gy * gz
    x, z = lax.axis_index("gx"), lax.axis_index("gz")

    turn = [(i * gy + j, j * gy + i) for i in range(gx) for j in range(gy)]
    turned = lax.ppermute(attn_out, ("gx", "gy"), turn)
    cut = turned.shape[1] // 2
    attn_cols = [
        lax.all_gather(turned[:, at:at + cut], "gy", axis=0, tiled=True) for at in (0, cut)
    ]

    def scattered(lefts, weight):
        done, total = 0, None
        for left in lefts:
            depth = left.shape[1]
            part = product(left, lax.slice_in_dim(weight, done, done + depth, axis=0))
            done += depth
            total = part if total is None else total + part

        def columns(zrel):
            def term(xrel):
                at = ((x ^ xrel) * rows, (z ^ zrel) * home)
                return lax.dynamic_slice(total, at, (rows, home))
            return reduced(term, "gx", gx)
        return reduced(columns, "gz", gz)

    projected = scattered(attn_cols, proj_weight)
    stream = residual.astype(jnp.float32) + projected
    scaled = (stream * norm_gain[None, :]).astype(jnp.bfloat16)
    squares = jnp.sum(stream * stream, axis=1)
    scaled = lax.all_gather(scaled, "gz", axis=1, tiled=True)
    scaled = lax.all_to_all(scaled, "gx", split_axis=1, concat_axis=0, tiled=True)
    for axis, size in (("gy", gy), ("gz", gz)):
        bit = 1
        while bit < size:
            squares = squares + swapped(squares, axis, size, bit)
            bit *= 2
    squares = lax.ppermute(squares, ("gx", "gy"), turn)
    inverse = lax.rsqrt(squares / width + 1e-05)[:, None]

    block = gate_proj.shape[1] // gx
    head = 3 * block // 7
    top = gx // 2

    def term_of(weight, at, size, left):
        def term(rel):
            return product(
                left, lax.dynamic_slice_in_dim(weight, (x ^ rel) * block + at, size, 1)
            )
        return term

    def far(at, size, left):
        return [
            halved(term_of(weight, at, size, left), "gx", gx, top, top).astype(jnp.bfloat16)
            for weight in (gate_proj, up_proj)
        ]

    def joined(at, size, left, arrived):
        parts = [
            (halved(term_of(weight, at, size, left), "gx", gx, top) + part.astype(jnp.float32))
            for weight, part in zip((gate_proj, up_proj), arrived)
        ]
        return jnp.concatenate([part.astype(jnp.bfloat16) for part in parts], axis=1)

    def activated(both):
        both = lax.psum_scatter(both, "gy", scatter_dimension=0, tiled=True).astype(jnp.float32)
        half = both.shape[1] // 2
        gate_sum, up_sum = inverse * both[:, :half], inverse * both[:, half:]
        piece = (jax.nn.silu(gate_sum) * up_sum).astype(jnp.bfloat16)
        return lax.all_gather(piece, "gy", axis=0, tiled=True)

    first = [swapped(part, "gx", gx, top) for part in far(0, head, scaled)]
    second = far(head, block - head, scaled)
    first, second = lax.optimization_barrier((first, second))
    second = [swapped(part, "gx", gx, top) for part in second]
    early = activated(joined(0, head, scaled, first))
    late = joined(head, block - head, scaled, second)
    early, late = lax.optimization_barrier((early, late))
    hidden = [early, activated(late)]

    down_sum = scattered(hidden, down_proj)
    return (stream + down_sum).astype(jnp.bfloat16)


def solution(mesh):
    sizes = tuple(mesh.shape[name] for name in ("gx", "gy", "gz"))
    in_specs = (
        P("gx", ("gz", "gy")),
        P("gx", ("gy", "gz")),
        P(("gz", "gx"), "gy"),
        P(("gy", "gz")),
        P(("gy", "gx"), "gz"),
        P(("gy", "gx"), "gz"),
        P(("gz", "gx"), "gy"),
    )
    out_specs = P("gx", ("gy", "gz"))
    return jax.shard_map(
        lambda *args: on_device(sizes, *args),
        mesh=mesh, in_specs=in_specs, out_specs=out_specs, check_vma=False,
    )
```

```python
import functools

import jax
import jax.numpy as jnp
from jax import lax
from jax.experimental import pallas as pl
from jax.experimental.pallas import tpu as pltpu
from jax.sharding import PartitionSpec as P

LANES = 128
MESH = pl.DeviceIdType.MESH


def product(left, right):
    return jnp.dot(left, right, preferred_element_type=jnp.float32)


def swapped(value, axis, size, bit):
    return lax.ppermute(value, axis, [(i, i ^ bit) for i in range(size)])


def halved(blocks, axis, size, bit, rel=0):
    if bit == 1:
        return blocks(rel)
    bit //= 2
    away = halved(blocks, axis, size, bit, rel | bit).astype(jnp.bfloat16)
    return halved(blocks, axis, size, bit, rel) + swapped(away, axis, size, bit).astype(jnp.float32)


def reduced(blocks, axis, size):
    return halved(blocks, axis, size, size)


def pick(index, values):
    out = values[-1]
    for i in range(len(values) - 2, -1, -1):
        out = jnp.where(index == i, values[i], out)
    return out


def relay_order(n):
    return [sorted((d for d in range(n) if d != r), key=lambda d: (-abs(d - r), (d - r) * (1 if r >= n // 2 else -1)))
            for r in range(n)]


def layer_kernel(
    n, chunk, width,
    attn, residual, gain, proj, gate, up, down, out,
    w, wd, att, atx, res, stream, scaled, gains, lhs, relay, xs, xr, zr, hid, acc, tmp, inv, sq, sqs,
    fs0, fr0, fsx, fsy, frx, fry, fsx2, fsy2, frx2, fry2,
    wl_sem, ws_sem, wr_sem, wd_sem, pl_sem, ps_sem, pr_sem, io_sem,
    al_sem, au_sem, ad_sem, ar_sem, ax_sem, axr_sem,
    cs_sem, cr_sem, rr_sem, qs_sem, qr_sem,
    xs_sem, xr_sem, zs_sem, zr_sem, us_sem, ds_sem, hr_sem, fs_sem, fr_sem,
):
    x, r, y = lax.axis_index("gx"), lax.axis_index("gy"), lax.axis_index("gz")
    core, xc = x % 2, x // 2
    other = x + 1 - 2 * core
    across = (x + 2) % 4
    rows, home = stream.shape
    half = home // 2
    depth = gate.shape[0]
    chunks = w.shape[1]
    hidden = chunks * chunk
    f32, bf16 = jnp.float32, jnp.bfloat16

    def at_x(i):
        return {"gx": i}

    y_other = {"gz": 1 - y}

    def send(src, dst, ssem, rsem, where):
        return pltpu.make_async_remote_copy(
            src_ref=src, dst_ref=dst, send_sem=ssem, recv_sem=rsem,
            device_id=where, device_id_type=MESH)

    def side(h):
        return pl.ds(h * half, half)

    own_proj = pl.ds(pl.multiple_of(core * home, home), home)
    for h in range(2):
        pltpu.make_async_copy(attn.at[:, side(h)], att.at[r, h], al_sem.at[h]).start()
    proj_in = pltpu.make_async_copy(proj, wd.at[own_proj, :], pl_sem)
    proj_in.start()
    res_in = pltpu.make_async_copy(residual, res, io_sem.at[0])
    res_in.start()
    gain_in = pltpu.make_async_copy(gain, gains, io_sem.at[1])
    gain_in.start()

    barrier = pltpu.get_barrier_semaphore()
    for where in (at_x(other), at_x(across), y_other):
        pl.semaphore_signal(barrier, inc=1, device_id=where, device_id_type=MESH)

    @pl.when(r < n - 1)
    def _():
        pl.semaphore_signal(barrier, inc=1, device_id={"gy": r + 1}, device_id_type=MESH)

    @pl.when(r > 0)
    def _():
        pl.semaphore_signal(barrier, inc=1, device_id={"gy": r - 1}, device_id_type=MESH)

    pl.semaphore_wait(barrier, 3 + jnp.where(r < n - 1, 1, 0) + jnp.where(r > 0, 1, 0))

    def a_up(s, h):
        return send(att.at[s, h], att.at[s, h], au_sem.at[s, h], ar_sem.at[s, h], {"gy": r + 1})

    def a_down(s, h):
        return send(att.at[s, h], att.at[s, h], ad_sem.at[s, h], ar_sem.at[s, h], {"gy": r - 1})

    def a_x(s, h):
        return send(att.at[s, h], atx.at[s % 2, h], ax_sem.at[s, h], axr_sem.at[s % 2, h], at_x(across))

    for h in range(2):
        pltpu.make_async_copy(attn.at[:, side(h)], att.at[r, h], al_sem.at[h]).wait()

        @pl.when(r < n - 1)
        def _():
            a_up(r, h).start()

        @pl.when(r > 0)
        def _():
            a_down(r, h).start()

        @pl.when(r // 2 != xc)
        def _():
            a_x(r, h).start()

    proj_out = send(proj, wd.at[own_proj, :], ps_sem, pr_sem, at_x(other))
    proj_out.start()

    def columns(q, k, c):
        place = xc if q == 0 else 1 - xc
        return pl.ds(pl.multiple_of((2 * place + c) * hidden + k * chunk, LANES), chunk)

    mine = pl.ds(pl.multiple_of(core * depth, depth), depth)
    theirs = pl.ds(pl.multiple_of((1 - core) * depth, depth), depth)

    def fetch(k, carry):
        for q in (1, 0):
            for part, src in ((0, gate), (1, up)):
                lanes = pl.ds(part * chunk, chunk)
                pltpu.make_async_copy(
                    src.at[:, columns(q, k, core)], w.at[q, k, mine, lanes], wl_sem.at[q, k]).start()
                send(src.at[:, columns(q, k, 1 - core)], w.at[q, k, mine, lanes],
                     ws_sem.at[q, k], wr_sem.at[q, k], at_x(other)).start()
        return carry

    def await_weights(q, k):
        pltpu.make_async_copy(w.at[q, k, mine, :], w.at[q, k, mine, :], wl_sem.at[q, k]).wait()
        send(w.at[q, k, theirs, :], w.at[q, k, theirs, :], ws_sem.at[q, k], wr_sem.at[q, k], at_x(other)).wait_recv()

    lax.fori_loop(0, chunks, fetch, 0)

    for step in range(1, n):
        for h in range(2):
            @pl.when(r >= step)
            def _():
                s = r - step
                a_up(s, h).wait_recv()

                @pl.when(r < n - 1)
                def _():
                    a_up(s, h).start()

                @pl.when(s // 2 != xc)
                def _():
                    a_x(s, h).start()

            @pl.when(r + step < n)
            def _():
                s = r + step
                a_down(s, h).wait_recv()

                @pl.when(r > 0)
                def _():
                    a_down(s, h).start()

                @pl.when(s // 2 != xc)
                def _():
                    a_x(s, h).start()

    proj_in.wait()
    proj_out.wait_recv()
    tile = 4 * LANES

    def project(rows_of, to):
        def body(j, carry):
            cols = pl.ds(pl.multiple_of(j * tile, tile), tile)
            value = None
            for i in range(2):
                for h in range(2):
                    term = product(rows_of(i, h), wd[i * home + h * half:i * home + (h + 1) * half, cols])
                    value = term if value is None else value + term
            acc[to, :, cols] = value
            return carry

        lax.fori_loop(0, acc.shape[2] // tile, body, 0)

    project(lambda i, h: att[2 * xc + i, h], xc)
    for h in range(2):
        for i in range(2):
            send(atx.at[i, h], atx.at[i, h], ax_sem.at[0, h], axr_sem.at[i, h], at_x(across)).wait_recv()
    project(lambda i, h: atx[i, h], 1 - xc)

    def copies():
        return (
            send(fsx, frx, fs_sem.at[1], fr_sem.at[1], at_x(across)),
            send(fsy, fry, fs_sem.at[2], fr_sem.at[2], y_other),
            send(fsx2, frx2, fs_sem.at[3], fr_sem.at[3], y_other),
            send(fsy2, fry2, fs_sem.at[4], fr_sem.at[4], at_x(across)),
        )

    def reduce_xy(part, finish):
        first_x, first_y, second_y, second_x = copies()
        for j in range(2):
            fsx[j] = part(1 - xc, j, 0).astype(bf16)
        first_x.start()
        for i in range(2):
            fsy[i] = part(i, 1 - y, 1).astype(bf16)
        first_y.start()
        first_x.wait_recv()
        fsx2[...] = (part(xc, 1 - y, 0) + frx[1 - y].astype(f32)).astype(bf16)
        second_y.start()
        first_y.wait_recv()
        fsy2[...] = (part(1 - xc, y, 1) + fry[1 - xc].astype(f32)).astype(bf16)
        second_x.start()
        second_y.wait_recv()
        finish(0, part(xc, y, 0) + frx[y].astype(f32) + frx2[...].astype(f32))
        second_x.wait_recv()
        finish(1, part(xc, y, 1) + fry[xc].astype(f32) + fry2[...].astype(f32))
        for copy in (first_x, first_y, second_y, second_x):
            copy.wait_send()

    same = xc == y

    def lanes_of(ref, slot, h):
        return ref.at[slot, :, side(h)]

    def to_partner(h):
        return send(scaled.at[h], lanes_of(lhs, x, h), cs_sem.at[0, h], cr_sem.at[x, h], at_x(other))

    def to_y(h):
        return send(scaled.at[h], lanes_of(lhs, x, h), cs_sem.at[1, h], cr_sem.at[x, h], y_other)

    def to_x(h):
        return send(scaled.at[h], lanes_of(lhs, x, h), cs_sem.at[0, h], cr_sem.at[x, h], at_x(across))

    def to_relay(h):
        return send(scaled.at[h], relay.at[h], cs_sem.at[1, h], rr_sem.at[h], y_other)

    def from_relay(h):
        return send(relay.at[h], lanes_of(lhs, x, h), cs_sem.at[2, h], cr_sem.at[x, h], at_x(across))

    def pass_own(h):
        return send(lanes_of(lhs, x, h), lanes_of(lhs, x, h), cs_sem.at[2, h], cr_sem.at[x, h], at_x(other))

    def pass_across(h):
        return send(lanes_of(lhs, across, h), lanes_of(lhs, across, h), cs_sem.at[3, h], cr_sem.at[across, h], at_x(other))

    def arrived(slot, h):
        send(lanes_of(lhs, slot, h), lanes_of(lhs, slot, h), cs_sem.at[3, h], cr_sem.at[slot, h], at_x(other)).wait_recv()

    def project_part(i, j, h):
        return acc[i, :, pl.ds(pl.multiple_of(j * home + h * half, LANES), half)]

    res_in.wait()
    gain_in.wait()

    def streamed(h, value):
        value = value + res[:, h * half:(h + 1) * half].astype(f32)
        stream[:, h * half:(h + 1) * half] = value
        value = (value * gains[:, h * half:(h + 1) * half]).astype(bf16)
        scaled[h] = value

        @pl.when(same)
        def _():
            to_y(h).start()
            to_partner(h).start()
            lhs[x, :, side(h)] = value

        @pl.when(jnp.logical_not(same))
        def _():
            to_relay(h).start()
            to_x(h).start()

    reduce_xy(project_part, streamed)

    for h in range(2):
        @pl.when(same)
        def _():
            send(relay.at[h], relay.at[h], cs_sem.at[1, h], rr_sem.at[h], y_other).wait_recv()
            from_relay(h).start()

        @pl.when(jnp.logical_not(same))
        def _():
            arrived(x, h)
            pass_own(h).start()

        arrived(across, h)
        pass_across(h).start()

    orders = relay_order(n)
    order = [pick(r, [orders[i][j] for i in range(n)]) for j in range(n - 1)]

    def send_piece(k, d):
        xs[k, d] = product(lhs[d], w[1, k]).astype(bf16)
        send(xs.at[k, d], xr.at[k, d], xs_sem, xr_sem.at[k, d], at_x(across)).start()

    def send_chunk(k):
        await_weights(1, k)
        for d in order + [r]:
            send_piece(k, d)

    def own_term(k, d):
        send(xr.at[k, d], xr.at[k, d], xs_sem, xr_sem.at[k, d], at_x(across)).wait_recv()
        return product(lhs[d], w[0, k]) + xr[k, d].astype(f32)

    def z_copy(k, d):
        ahead = d > r
        nxt = jnp.where(ahead, r + 1, r - 1)
        place = jnp.where(jnp.logical_and(jnp.logical_not(ahead), d == r - 1), n, d)
        return send(xr.at[k, d], zr.at[k, place], zs_sem.at[k, d], zr_sem.at[k, place], {"gy": nxt})

    def z_wait(k, place):
        send(zr.at[k, place], zr.at[k, place], zs_sem.at[k, 0], zr_sem.at[k, place], {"gy": r}).wait_recv()

    def relay_chunk(k):
        await_weights(0, k)
        for d in order:
            tmp[...] = own_term(k, d)
            inner = jnp.logical_or(jnp.logical_and(d > r, r > 0), jnp.logical_and(d < r, r < n - 1))

            @pl.when(inner)
            def _():
                z_wait(k, d)
                tmp[...] = tmp[...] + zr[k, d].astype(f32)

            xr[k, d] = tmp[...].astype(bf16)
            z_copy(k, d).start()

    def up_copy(k, s):
        return send(hid.at[k, s], hid.at[k, s], us_sem.at[k, s], hr_sem.at[k, s], {"gy": r + 1})

    def down_copy(k, s):
        return send(hid.at[k, s], hid.at[k, s], ds_sem.at[k, s], hr_sem.at[k, s], {"gy": r - 1})

    def down_rows(k):
        return pl.ds(pl.multiple_of(k * chunk, chunk), chunk)

    def contract(k, s):
        acc[s] = acc[s] + product(hid[k, s], wd[down_rows(k), :])

    def finish_chunk(k):
        tmp[...] = own_term(k, r)

        @pl.when(r > 0)
        def _():
            z_wait(k, r)
            tmp[...] = tmp[...] + zr[k, r].astype(f32)

        @pl.when(r < n - 1)
        def _():
            z_wait(k, n)
            tmp[...] = tmp[...] + zr[k, n].astype(f32)

        gate_sum = inv[...] * tmp[:, :chunk]
        up_sum = inv[...] * tmp[:, chunk:]
        hid[k, r] = (gate_sum / (1.0 + jnp.exp(-gate_sum)) * up_sum).astype(bf16)

        @pl.when(r < n - 1)
        def _():
            up_copy(k, r).start()

        @pl.when(r > 0)
        def _():
            down_copy(k, r).start()

        pltpu.make_async_copy(wd.at[down_rows(k), :], wd.at[down_rows(k), :], wd_sem.at[k]).wait()
        contract(k, r)

    def pass_chunk(k, step):
        @pl.when(r >= step)
        def _():
            up_copy(k, r - step).wait_recv()

            @pl.when(r < n - 1)
            def _():
                up_copy(k, r - step).start()

            contract(k, r - step)

        @pl.when(r + step < n)
        def _():
            down_copy(k, r + step).wait_recv()

            @pl.when(r > 0)
            def _():
                down_copy(k, r + step).start()

            contract(k, r + step)

    third = (other + 2) % 4
    await_weights(1, 0)
    send_piece(0, x)
    send_piece(0, across)
    for d in (other, third):
        for h in range(2):
            arrived(d, h)
        send_piece(0, d)

    slot = r * 2 + y

    def sq_copy(ox, oy):
        return send(sq, sqs.at[slot], qs_sem.at[ox, oy], qr_sem.at[slot],
                    ((x + ox) % 4, x, (y + oy) % 2))

    own_squares = r == x
    sq[...] = jnp.zeros_like(sq)
    squares = stream[...] * stream[...]
    sq[:, :rows] = lax.dot_general(
        jnp.ones((sq.shape[0], home), f32), squares, (((1,), (1,)), ((), ())),
        precision=lax.Precision.HIGHEST, preferred_element_type=f32)

    @pl.when(own_squares)
    def _():
        sqs[slot] = sq[...]

    @pl.when(jnp.logical_not(own_squares))
    def _():
        sq_copy(0, 0).start()

    for ox in range(4):
        for oy in range(2):
            if ox or oy:
                sq_copy(ox, oy).start()

    def fetch_down(k, carry):
        place = pl.ds(pl.multiple_of(k * chunk, chunk), chunk)
        pltpu.make_async_copy(down.at[place, :], wd.at[place, :], wd_sem.at[k]).start()
        return carry

    lax.fori_loop(0, chunks, fetch_down, 0)
    acc[...] = jnp.zeros_like(acc)

    send_chunk(1)

    for i in range(2 * n):
        own = jnp.logical_and(x == r, slot == i)

        @pl.when(jnp.logical_not(own))
        def _():
            send(sqs.at[i], sqs.at[i], qs_sem.at[0, 0], qr_sem.at[i], y_other).wait_recv()

    summed = sqs[0]
    for i in range(1, 2 * n):
        summed = summed + sqs[i]
    inverse = lax.rsqrt(summed / width + 1e-05) * (1.0 / summed.shape[0])
    spread = lax.dot_general(
        inverse, jnp.ones((summed.shape[0], chunk), f32), (((0,), (0,)), ((), ())),
        precision=lax.Precision.HIGHEST, preferred_element_type=f32)
    inv[...] = spread[:rows]

    def body(t, carry):
        @pl.when(t + 2 < chunks)
        def _():
            send_chunk(t + 2)

        @pl.when(t < chunks)
        def _():
            relay_chunk(t)

        @pl.when(jnp.logical_and(t >= 1, t <= chunks))
        def _():
            finish_chunk(t - 1)

        for step in range(1, n):
            k = t - 1 - 2 * step

            @pl.when(jnp.logical_and(k >= 0, k < chunks))
            def _():
                pass_chunk(k, step)

        return carry

    lax.fori_loop(0, chunks + 2 * n, body, 0)

    for i in range(2):
        fs0[i] = acc[2 * i + 1 - core].astype(bf16)
    swap = send(fs0, fr0, fs_sem.at[0], fr_sem.at[0], at_x(other))
    swap.start()
    swap.wait_recv()

    def down_part(i, j, h):
        cols = pl.ds(pl.multiple_of(j * home + h * half, LANES), half)
        return acc[2 * i + core, :, cols] + fr0[i, :, cols].astype(f32)

    def written(h, value):
        out[:, h * half:(h + 1) * half] = (stream[:, h * half:(h + 1) * half] + value).astype(bf16)

    reduce_xy(down_part, written)

    swap.wait_send()
    proj_out.wait_send()
    send(xs, xs, xs_sem, xr_sem.at[0, 0], at_x(across)).wait_send()

    for h in range(2):
        @pl.when(same)
        def _():
            to_y(h).wait_send()
            to_partner(h).wait_send()
            from_relay(h).wait_send()

        @pl.when(jnp.logical_not(same))
        def _():
            to_relay(h).wait_send()
            to_x(h).wait_send()
            pass_own(h).wait_send()

        pass_across(h).wait_send()

        for s in range(n):
            @pl.when(jnp.logical_and(s <= r, r < n - 1))
            def _():
                a_up(s, h).wait_send()

            @pl.when(jnp.logical_and(s >= r, r > 0))
            def _():
                a_down(s, h).wait_send()

            @pl.when(s // 2 != xc)
            def _():
                a_x(s, h).wait_send()

    @pl.when(jnp.logical_not(own_squares))
    def _():
        sq_copy(0, 0).wait_send()

    for ox in range(4):
        for oy in range(2):
            if ox or oy:
                sq_copy(ox, oy).wait_send()

    def drain(k, carry):
        for q in range(2):
            send(w.at[q, k, mine, :], w.at[q, k, mine, :], ws_sem.at[q, k], wr_sem.at[q, k], at_x(other)).wait_send()
        for d in order:
            z_copy(k, d).wait_send()

        for s in range(n):
            @pl.when(jnp.logical_and(s <= r, r < n - 1))
            def _():
                up_copy(k, s).wait_send()

            @pl.when(jnp.logical_and(s >= r, r > 0))
            def _():
                down_copy(k, s).wait_send()

        return carry

    lax.fori_loop(0, chunks, drain, 0)


def layer(sizes, attn_out, residual, proj_weight, norm_gain, gate_proj, up_proj, down_proj):
    gx, n, gz = sizes
    rows, home = residual.shape
    depth = gate_proj.shape[0]
    hidden = gate_proj.shape[1] // gx
    width = home * n * gz
    chunk = LANES
    chunks = hidden // chunk
    cols = down_proj.shape[1]
    half = home // 2
    lanes = -(-rows // LANES) * LANES
    bf16, f32 = jnp.bfloat16, jnp.float32
    dma, vm = pltpu.SemaphoreType.DMA, pltpu.VMEM
    scratch = [
        vm((2, chunks, 2 * depth, 2 * chunk), bf16),
        vm((max(2 * home, hidden), cols), bf16),
        vm((n, 2, rows, half), bf16),
        vm((2, 2, rows, half), bf16),
        vm((rows, home), bf16),
        vm((rows, home), f32),
        vm((2, rows, half), bf16),
        vm((1, home), f32),
        vm((gx, rows, home), bf16),
        vm((2, rows, half), bf16),
        vm((chunks, n, rows, 2 * chunk), bf16),
        vm((chunks, n, rows, 2 * chunk), bf16),
        vm((chunks, n + 1, rows, 2 * chunk), bf16),
        vm((chunks, n, rows, chunk), bf16),
        vm((n, rows, cols), f32),
        vm((rows, 2 * chunk), f32),
        vm((rows, chunk), f32),
        vm((8, lanes), f32),
        vm((2 * n, 8, lanes), f32),
        vm((2, rows, cols), bf16), vm((2, rows, cols), bf16),
        vm((2, rows, half), bf16), vm((2, rows, half), bf16),
        vm((2, rows, half), bf16), vm((2, rows, half), bf16),
        vm((rows, half), bf16), vm((rows, half), bf16),
        vm((rows, half), bf16), vm((rows, half), bf16),
        dma((2, chunks)), dma((2, chunks)), dma((2, chunks)), dma((chunks,)),
        dma, dma, dma, dma((2,)),
        dma((2,)), dma((n, 2)), dma((n, 2)), dma((n, 2)), dma((n, 2)), dma((2, 2)),
        dma((4, 2)), dma((gx, 2)), dma((2,)), dma((gx, gz)), dma((2 * n,)),
        dma, dma((chunks, n)), dma((chunks, n)), dma((chunks, n + 1)),
        dma((chunks, n)), dma((chunks, n)), dma((chunks, n)), dma((5,)), dma((5,)),
    ]
    away = pl.BlockSpec(memory_space=pl.ANY)
    return pl.pallas_call(
        functools.partial(layer_kernel, n, chunk, width),
        out_shape=jax.ShapeDtypeStruct((rows, home), bf16),
        in_specs=[away] * 7,
        out_specs=pl.BlockSpec(memory_space=pltpu.VMEM),
        scratch_shapes=scratch,
        compiler_params=pltpu.CompilerParams(
            collective_id=0, has_side_effects=True, vmem_limit_bytes=67043328),
    )(attn_out, residual, norm_gain[None, :], proj_weight, gate_proj, up_proj, down_proj)


def on_device(sizes, attn_out, residual, proj_weight, norm_gain, gate_proj, up_proj, down_proj):
    gx, gy, gz = sizes
    assert gx == gy
    if gx == 4 and gz == 2:
        return layer(sizes, attn_out, residual, proj_weight, norm_gain, gate_proj, up_proj, down_proj)
    rows, home = residual.shape
    width = home * gy * gz
    x, z = lax.axis_index("gx"), lax.axis_index("gz")

    turn = [(i * gy + j, j * gy + i) for i in range(gx) for j in range(gy)]
    turned = lax.ppermute(attn_out, ("gx", "gy"), turn)
    cut = turned.shape[1] // 2
    attn_cols = [
        lax.all_gather(turned[:, at:at + cut], "gy", axis=0, tiled=True) for at in (0, cut)
    ]

    def scattered(lefts, weight):
        done, total = 0, None
        for left in lefts:
            depth = left.shape[1]
            part = product(left, lax.slice_in_dim(weight, done, done + depth, axis=0))
            done += depth
            total = part if total is None else total + part

        def columns(zrel):
            def term(xrel):
                at = ((x ^ xrel) * rows, (z ^ zrel) * home)
                return lax.dynamic_slice(total, at, (rows, home))
            return reduced(term, "gx", gx)
        return reduced(columns, "gz", gz)

    projected = scattered(attn_cols, proj_weight)
    stream = residual.astype(jnp.float32) + projected
    scaled = (stream * norm_gain[None, :]).astype(jnp.bfloat16)
    squares = jnp.sum(stream * stream, axis=1)
    scaled = lax.all_gather(scaled, "gz", axis=1, tiled=True)
    scaled = lax.all_to_all(scaled, "gx", split_axis=1, concat_axis=0, tiled=True)
    for axis, size in (("gy", gy), ("gz", gz)):
        bit = 1
        while bit < size:
            squares = squares + swapped(squares, axis, size, bit)
            bit *= 2
    squares = lax.ppermute(squares, ("gx", "gy"), turn)
    inverse = lax.rsqrt(squares / width + 1e-05)[:, None]

    block = gate_proj.shape[1] // gx
    head = 3 * block // 7
    top = gx // 2

    def term_of(weight, at, size, left):
        def term(rel):
            return product(
                left, lax.dynamic_slice_in_dim(weight, (x ^ rel) * block + at, size, 1)
            )
        return term

    def far(at, size, left):
        return [
            halved(term_of(weight, at, size, left), "gx", gx, top, top).astype(jnp.bfloat16)
            for weight in (gate_proj, up_proj)
        ]

    def joined(at, size, left, arrived):
        parts = [
            (halved(term_of(weight, at, size, left), "gx", gx, top) + part.astype(jnp.float32))
            for weight, part in zip((gate_proj, up_proj), arrived)
        ]
        return jnp.concatenate([part.astype(jnp.bfloat16) for part in parts], axis=1)

    def activated(both):
        both = lax.psum_scatter(both, "gy", scatter_dimension=0, tiled=True).astype(jnp.float32)
        half = both.shape[1] // 2
        gate_sum, up_sum = inverse * both[:, :half], inverse * both[:, half:]
        piece = (jax.nn.silu(gate_sum) * up_sum).astype(jnp.bfloat16)
        return lax.all_gather(piece, "gy", axis=0, tiled=True)

    first = [swapped(part, "gx", gx, top) for part in far(0, head, scaled)]
    second = far(head, block - head, scaled)
    first, second = lax.optimization_barrier((first, second))
    second = [swapped(part, "gx", gx, top) for part in second]
    early = activated(joined(0, head, scaled, first))
    late = joined(head, block - head, scaled, second)
    early, late = lax.optimization_barrier((early, late))
    hidden = [early, activated(late)]

    down_sum = scattered(hidden, down_proj)
    return (stream + down_sum).astype(jnp.bfloat16)


def solution(mesh):
    sizes = tuple(mesh.shape[name] for name in ("gx", "gy", "gz"))
    in_specs = (
        P("gx", ("gz", "gy")),
        P("gx", ("gy", "gz")),
        P(("gz", "gx"), "gy"),
        P(("gy", "gz")),
        P(("gy", "gx"), "gz"),
        P(("gy", "gx"), "gz"),
        P(("gz", "gx"), "gy"),
    )
    out_specs = P("gx", ("gy", "gz"))
    return jax.shard_map(
        lambda *args: on_device(sizes, *args),
        mesh=mesh, in_specs=in_specs, out_specs=out_specs, check_vma=False,
    )
```

```python
import functools

import jax
import jax.numpy as jnp
from jax import lax
from jax.experimental import pallas as pl
from jax.experimental.pallas import tpu as pltpu
from jax.sharding import PartitionSpec as P

LANES = 128
MESH = pl.DeviceIdType.MESH


def product(left, right):
    return jnp.dot(left, right, preferred_element_type=jnp.float32)


def swapped(value, axis, size, bit):
    return lax.ppermute(value, axis, [(i, i ^ bit) for i in range(size)])


def halved(blocks, axis, size, bit, rel=0):
    if bit == 1:
        return blocks(rel)
    bit //= 2
    away = halved(blocks, axis, size, bit, rel | bit).astype(jnp.bfloat16)
    return halved(blocks, axis, size, bit, rel) + swapped(away, axis, size, bit).astype(jnp.float32)


def reduced(blocks, axis, size):
    return halved(blocks, axis, size, size)


def pick(index, values):
    out = values[-1]
    for i in range(len(values) - 2, -1, -1):
        out = jnp.where(index == i, values[i], out)
    return out


def relay_order(n):
    return [sorted((d for d in range(n) if d != r), key=lambda d: (-abs(d - r), (d - r) * (1 if r >= n // 2 else -1)))
            for r in range(n)]


def layer_kernel(
    n, chunk, width,
    attn, residual, gain, proj, gate, up, down, out,
    w, wd, att, atx, res, stream, scaled, gains, lhs, relay, xs, xr, zr, hid, acc, tmp, inv, sq, sqs,
    fs0, fr0, fsx, fsy, frx, fry, fsx2, fsy2, frx2, fry2,
    wl_sem, ws_sem, wr_sem, wd_sem, pl_sem, ps_sem, pr_sem, io_sem,
    al_sem, au_sem, ad_sem, ar_sem, ax_sem, axr_sem,
    cs_sem, cr_sem, rr_sem, qs_sem, qr_sem,
    xs_sem, xr_sem, zs_sem, zr_sem, us_sem, ds_sem, hr_sem, fs_sem, fr_sem,
):
    x, r, y = lax.axis_index("gx"), lax.axis_index("gy"), lax.axis_index("gz")
    core, xc = x % 2, x // 2
    other = x + 1 - 2 * core
    across = (x + 2) % 4
    rows, home = stream.shape
    half = home // 2
    depth = gate.shape[0]
    chunks = w.shape[1]
    hidden = chunks * chunk
    f32, bf16 = jnp.float32, jnp.bfloat16

    def at_x(i):
        return {"gx": i}

    y_other = {"gz": 1 - y}

    def send(src, dst, ssem, rsem, where):
        return pltpu.make_async_remote_copy(
            src_ref=src, dst_ref=dst, send_sem=ssem, recv_sem=rsem,
            device_id=where, device_id_type=MESH)

    def side(h):
        return pl.ds(h * half, half)

    own_proj = pl.ds(pl.multiple_of(core * home, home), home)
    for h in range(2):
        pltpu.make_async_copy(attn.at[:, side(h)], att.at[r, h], al_sem.at[h]).start()
    proj_in = pltpu.make_async_copy(proj, wd.at[own_proj, :], pl_sem)
    proj_in.start()
    res_in = pltpu.make_async_copy(residual, res, io_sem.at[0])
    res_in.start()
    gain_in = pltpu.make_async_copy(gain, gains, io_sem.at[1])
    gain_in.start()

    barrier = pltpu.get_barrier_semaphore()
    for where in (at_x(other), at_x(across), y_other):
        pl.semaphore_signal(barrier, inc=1, device_id=where, device_id_type=MESH)

    @pl.when(r < n - 1)
    def _():
        pl.semaphore_signal(barrier, inc=1, device_id={"gy": r + 1}, device_id_type=MESH)

    @pl.when(r > 0)
    def _():
        pl.semaphore_signal(barrier, inc=1, device_id={"gy": r - 1}, device_id_type=MESH)

    pl.semaphore_wait(barrier, 3 + jnp.where(r < n - 1, 1, 0) + jnp.where(r > 0, 1, 0))

    def a_up(s, h):
        return send(att.at[s, h], att.at[s, h], au_sem.at[s, h], ar_sem.at[s, h], {"gy": r + 1})

    def a_down(s, h):
        return send(att.at[s, h], att.at[s, h], ad_sem.at[s, h], ar_sem.at[s, h], {"gy": r - 1})

    def a_x(s, h):
        return send(att.at[s, h], atx.at[s % 2, h], ax_sem.at[s, h], axr_sem.at[s % 2, h], at_x(across))

    for h in range(2):
        pltpu.make_async_copy(attn.at[:, side(h)], att.at[r, h], al_sem.at[h]).wait()

        @pl.when(r < n - 1)
        def _():
            a_up(r, h).start()

        @pl.when(r > 0)
        def _():
            a_down(r, h).start()

        @pl.when(r // 2 != xc)
        def _():
            a_x(r, h).start()

    proj_out = send(proj, wd.at[own_proj, :], ps_sem, pr_sem, at_x(other))
    proj_out.start()

    def columns(q, k, c):
        place = xc if q == 0 else 1 - xc
        return pl.ds(pl.multiple_of((2 * place + c) * hidden + k * chunk, LANES), chunk)

    mine = pl.ds(pl.multiple_of(core * depth, depth), depth)
    theirs = pl.ds(pl.multiple_of((1 - core) * depth, depth), depth)

    def fetch(k, carry):
        for q in (1, 0):
            for part, src in ((0, gate), (1, up)):
                lanes = pl.ds(part * chunk, chunk)
                pltpu.make_async_copy(
                    src.at[:, columns(q, k, core)], w.at[q, k, mine, lanes], wl_sem.at[q, k]).start()
                send(src.at[:, columns(q, k, 1 - core)], w.at[q, k, mine, lanes],
                     ws_sem.at[q, k], wr_sem.at[q, k], at_x(other)).start()
        return carry

    def await_weights(q, k):
        pltpu.make_async_copy(w.at[q, k, mine, :], w.at[q, k, mine, :], wl_sem.at[q, k]).wait()
        send(w.at[q, k, theirs, :], w.at[q, k, theirs, :], ws_sem.at[q, k], wr_sem.at[q, k], at_x(other)).wait_recv()

    lax.fori_loop(0, chunks, fetch, 0)

    for step in range(1, n):
        for h in range(2):
            @pl.when(r >= step)
            def _():
                s = r - step
                a_up(s, h).wait_recv()

                @pl.when(r < n - 1)
                def _():
                    a_up(s, h).start()

                @pl.when(s // 2 != xc)
                def _():
                    a_x(s, h).start()

            @pl.when(r + step < n)
            def _():
                s = r + step
                a_down(s, h).wait_recv()

                @pl.when(r > 0)
                def _():
                    a_down(s, h).start()

                @pl.when(s // 2 != xc)
                def _():
                    a_x(s, h).start()

    proj_in.wait()
    proj_out.wait_recv()
    tile = 4 * LANES

    def project(rows_of, to):
        def body(j, carry):
            cols = pl.ds(pl.multiple_of(j * tile, tile), tile)
            value = None
            for i in range(2):
                for h in range(2):
                    term = product(rows_of(i, h), wd[i * home + h * half:i * home + (h + 1) * half, cols])
                    value = term if value is None else value + term
            acc[to, :, cols] = value
            return carry

        lax.fori_loop(0, acc.shape[2] // tile, body, 0)

    project(lambda i, h: att[2 * xc + i, h], xc)
    for h in range(2):
        for i in range(2):
            send(atx.at[i, h], atx.at[i, h], ax_sem.at[0, h], axr_sem.at[i, h], at_x(across)).wait_recv()
    project(lambda i, h: atx[i, h], 1 - xc)

    def copies():
        def over_x(j, at):
            return send(fsx.at[j], frx.at[j], fs_sem.at[at], fr_sem.at[at], at_x(across))

        def over_y(i, at):
            return send(fsy.at[i], fry.at[i], fs_sem.at[at], fr_sem.at[at], y_other)

        return (
            over_x(1 - y, 2), over_x(y, 3), over_y(1 - xc, 4), over_y(xc, 5),
            send(fsx2, frx2, fs_sem.at[6], fr_sem.at[6], y_other),
            send(fsy2, fry2, fs_sem.at[7], fr_sem.at[7], at_x(across)),
        )

    def reduce_xy(part, finish, leaving=lambda: None, staying=lambda: None):
        x_next, x_last, y_next, y_last, second_y, second_x = copies()
        leaving()
        fsx[1 - y] = part(1 - xc, 1 - y, 0).astype(bf16)
        x_next.start()
        fsy[1 - xc] = part(1 - xc, 1 - y, 1).astype(bf16)
        y_next.start()
        fsx[y] = part(1 - xc, y, 0).astype(bf16)
        x_last.start()
        staying()
        fsy[xc] = part(xc, 1 - y, 1).astype(bf16)
        y_last.start()
        x_next.wait_recv()
        fsx2[...] = (part(xc, 1 - y, 0) + frx[1 - y].astype(f32)).astype(bf16)
        second_y.start()
        y_next.wait_recv()
        fsy2[...] = (part(1 - xc, y, 1) + fry[1 - xc].astype(f32)).astype(bf16)
        second_x.start()
        x_last.wait_recv()
        second_y.wait_recv()
        finish(0, part(xc, y, 0) + frx[y].astype(f32) + frx2[...].astype(f32))
        y_last.wait_recv()
        second_x.wait_recv()
        finish(1, part(xc, y, 1) + fry[xc].astype(f32) + fry2[...].astype(f32))
        for copy in (x_next, x_last, y_next, y_last, second_y, second_x):
            copy.wait_send()

    same = xc == y

    def lanes_of(ref, slot, h):
        return ref.at[slot, :, side(h)]

    def to_partner(h):
        return send(scaled.at[h], lanes_of(lhs, x, h), cs_sem.at[0, h], cr_sem.at[x, h], at_x(other))

    def to_y(h):
        return send(scaled.at[h], lanes_of(lhs, x, h), cs_sem.at[1, h], cr_sem.at[x, h], y_other)

    def to_x(h):
        return send(scaled.at[h], lanes_of(lhs, x, h), cs_sem.at[0, h], cr_sem.at[x, h], at_x(across))

    def to_relay(h):
        return send(scaled.at[h], relay.at[h], cs_sem.at[1, h], rr_sem.at[h], y_other)

    def from_relay(h):
        return send(relay.at[h], lanes_of(lhs, x, h), cs_sem.at[2, h], cr_sem.at[x, h], at_x(across))

    def pass_own(h):
        return send(lanes_of(lhs, x, h), lanes_of(lhs, x, h), cs_sem.at[2, h], cr_sem.at[x, h], at_x(other))

    def pass_across(h):
        return send(lanes_of(lhs, across, h), lanes_of(lhs, across, h), cs_sem.at[3, h], cr_sem.at[across, h], at_x(other))

    def arrived(slot, h):
        send(lanes_of(lhs, slot, h), lanes_of(lhs, slot, h), cs_sem.at[3, h], cr_sem.at[slot, h], at_x(other)).wait_recv()

    def project_part(i, j, h):
        return acc[i, :, pl.ds(pl.multiple_of(j * home + h * half, LANES), half)]

    res_in.wait()
    gain_in.wait()

    def streamed(h, value):
        value = value + res[:, h * half:(h + 1) * half].astype(f32)
        stream[:, h * half:(h + 1) * half] = value
        value = (value * gains[:, h * half:(h + 1) * half]).astype(bf16)
        scaled[h] = value

        @pl.when(same)
        def _():
            to_y(h).start()
            to_partner(h).start()
            lhs[x, :, side(h)] = value

        @pl.when(jnp.logical_not(same))
        def _():
            to_relay(h).start()
            to_x(h).start()

    reduce_xy(project_part, streamed)

    for h in range(2):
        @pl.when(same)
        def _():
            send(relay.at[h], relay.at[h], cs_sem.at[1, h], rr_sem.at[h], y_other).wait_recv()
            from_relay(h).start()

        @pl.when(jnp.logical_not(same))
        def _():
            arrived(x, h)
            pass_own(h).start()

        arrived(across, h)
        pass_across(h).start()

    orders = relay_order(n)
    order = [pick(r, [orders[i][j] for i in range(n)]) for j in range(n - 1)]

    def send_piece(k, d):
        xs[k, d] = product(lhs[d], w[1, k]).astype(bf16)
        send(xs.at[k, d], xr.at[k, d], xs_sem, xr_sem.at[k, d], at_x(across)).start()

    def send_chunk(k):
        await_weights(1, k)
        for d in order + [r]:
            send_piece(k, d)

    def own_term(k, d):
        send(xr.at[k, d], xr.at[k, d], xs_sem, xr_sem.at[k, d], at_x(across)).wait_recv()
        return product(lhs[d], w[0, k]) + xr[k, d].astype(f32)

    def z_copy(k, d):
        ahead = d > r
        nxt = jnp.where(ahead, r + 1, r - 1)
        place = jnp.where(jnp.logical_and(jnp.logical_not(ahead), d == r - 1), n, d)
        return send(xr.at[k, d], zr.at[k, place], zs_sem.at[k, d], zr_sem.at[k, place], {"gy": nxt})

    def z_wait(k, place):
        send(zr.at[k, place], zr.at[k, place], zs_sem.at[k, 0], zr_sem.at[k, place], {"gy": r}).wait_recv()

    def relay_chunk(k):
        await_weights(0, k)
        for d in order:
            tmp[...] = own_term(k, d)
            inner = jnp.logical_or(jnp.logical_and(d > r, r > 0), jnp.logical_and(d < r, r < n - 1))

            @pl.when(inner)
            def _():
                z_wait(k, d)
                tmp[...] = tmp[...] + zr[k, d].astype(f32)

            xr[k, d] = tmp[...].astype(bf16)
            z_copy(k, d).start()

    def up_copy(k, s):
        return send(hid.at[k, s], hid.at[k, s], us_sem.at[k, s], hr_sem.at[k, s], {"gy": r + 1})

    def down_copy(k, s):
        return send(hid.at[k, s], hid.at[k, s], ds_sem.at[k, s], hr_sem.at[k, s], {"gy": r - 1})

    def down_rows(k):
        return pl.ds(pl.multiple_of(k * chunk, chunk), chunk)

    def contract(k, s):
        acc[s] = acc[s] + product(hid[k, s], wd[down_rows(k), :])

    def finish_chunk(k):
        tmp[...] = own_term(k, r)

        @pl.when(r > 0)
        def _():
            z_wait(k, r)
            tmp[...] = tmp[...] + zr[k, r].astype(f32)

        @pl.when(r < n - 1)
        def _():
            z_wait(k, n)
            tmp[...] = tmp[...] + zr[k, n].astype(f32)

        gate_sum = inv[...] * tmp[:, :chunk]
        up_sum = inv[...] * tmp[:, chunk:]
        hid[k, r] = (gate_sum / (1.0 + jnp.exp(-gate_sum)) * up_sum).astype(bf16)

        @pl.when(r < n - 1)
        def _():
            up_copy(k, r).start()

        @pl.when(r > 0)
        def _():
            down_copy(k, r).start()

        pltpu.make_async_copy(wd.at[down_rows(k), :], wd.at[down_rows(k), :], wd_sem.at[k]).wait()
        contract(k, r)

    def pass_chunk(k, step):
        @pl.when(r >= step)
        def _():
            up_copy(k, r - step).wait_recv()

            @pl.when(r < n - 1)
            def _():
                up_copy(k, r - step).start()

            contract(k, r - step)

        @pl.when(r + step < n)
        def _():
            down_copy(k, r + step).wait_recv()

            @pl.when(r > 0)
            def _():
                down_copy(k, r + step).start()

            contract(k, r + step)

    third = (other + 2) % 4
    await_weights(1, 0)
    send_piece(0, x)
    send_piece(0, across)
    for d in (other, third):
        for h in range(2):
            arrived(d, h)
        send_piece(0, d)

    slot = r * 2 + y

    def sq_copy(ox, oy):
        return send(sq, sqs.at[slot], qs_sem.at[ox, oy], qr_sem.at[slot],
                    ((x + ox) % 4, x, (y + oy) % 2))

    own_squares = r == x
    sq[...] = jnp.zeros_like(sq)
    squares = stream[...] * stream[...]
    sq[:, :rows] = lax.dot_general(
        jnp.ones((sq.shape[0], home), f32), squares, (((1,), (1,)), ((), ())),
        precision=lax.Precision.HIGHEST, preferred_element_type=f32)

    @pl.when(own_squares)
    def _():
        sqs[slot] = sq[...]

    @pl.when(jnp.logical_not(own_squares))
    def _():
        sq_copy(0, 0).start()

    for ox in range(4):
        for oy in range(2):
            if ox or oy:
                sq_copy(ox, oy).start()

    def fetch_down(k, carry):
        place = pl.ds(pl.multiple_of(k * chunk, chunk), chunk)
        pltpu.make_async_copy(down.at[place, :], wd.at[place, :], wd_sem.at[k]).start()
        return carry

    lax.fori_loop(0, chunks, fetch_down, 0)
    acc[...] = jnp.zeros_like(acc)

    send_chunk(1)

    for i in range(2 * n):
        own = jnp.logical_and(x == r, slot == i)

        @pl.when(jnp.logical_not(own))
        def _():
            send(sqs.at[i], sqs.at[i], qs_sem.at[0, 0], qr_sem.at[i], y_other).wait_recv()

    summed = sqs[0]
    for i in range(1, 2 * n):
        summed = summed + sqs[i]
    inverse = lax.rsqrt(summed / width + 1e-05) * (1.0 / summed.shape[0])
    spread = lax.dot_general(
        inverse, jnp.ones((summed.shape[0], chunk), f32), (((0,), (0,)), ((), ())),
        precision=lax.Precision.HIGHEST, preferred_element_type=f32)
    inv[...] = spread[:rows]

    def body(t, carry):
        @pl.when(t + 2 < chunks)
        def _():
            send_chunk(t + 2)

        @pl.when(t < chunks)
        def _():
            relay_chunk(t)

        @pl.when(jnp.logical_and(t >= 1, t <= chunks))
        def _():
            finish_chunk(t - 1)

        for step in range(1, n):
            k = t - 1 - 2 * step

            @pl.when(jnp.logical_and(k >= 0, k < chunks))
            def _():
                pass_chunk(k, step)

        return carry

    lax.fori_loop(0, chunks + 2 * n, body, 0)

    def swap(i, at):
        return send(fs0.at[i], fr0.at[i], fs_sem.at[at], fr_sem.at[at], at_x(other))

    swaps = (swap(1 - xc, 0), swap(xc, 1))
    for i, copy in zip((1 - xc, xc), swaps):
        fs0[i] = acc[2 * i + 1 - core].astype(bf16)
        copy.start()

    def down_part(i, j, h):
        cols = pl.ds(pl.multiple_of(j * home + h * half, LANES), half)
        return acc[2 * i + core, :, cols] + fr0[i, :, cols].astype(f32)

    def written(h, value):
        out[:, h * half:(h + 1) * half] = (stream[:, h * half:(h + 1) * half] + value).astype(bf16)

    reduce_xy(down_part, written, swaps[0].wait_recv, swaps[1].wait_recv)

    for copy in swaps:
        copy.wait_send()
    proj_out.wait_send()
    send(xs, xs, xs_sem, xr_sem.at[0, 0], at_x(across)).wait_send()

    for h in range(2):
        @pl.when(same)
        def _():
            to_y(h).wait_send()
            to_partner(h).wait_send()
            from_relay(h).wait_send()

        @pl.when(jnp.logical_not(same))
        def _():
            to_relay(h).wait_send()
            to_x(h).wait_send()
            pass_own(h).wait_send()

        pass_across(h).wait_send()

        for s in range(n):
            @pl.when(jnp.logical_and(s <= r, r < n - 1))
            def _():
                a_up(s, h).wait_send()

            @pl.when(jnp.logical_and(s >= r, r > 0))
            def _():
                a_down(s, h).wait_send()

            @pl.when(s // 2 != xc)
            def _():
                a_x(s, h).wait_send()

    @pl.when(jnp.logical_not(own_squares))
    def _():
        sq_copy(0, 0).wait_send()

    for ox in range(4):
        for oy in range(2):
            if ox or oy:
                sq_copy(ox, oy).wait_send()

    def drain(k, carry):
        for q in range(2):
            send(w.at[q, k, mine, :], w.at[q, k, mine, :], ws_sem.at[q, k], wr_sem.at[q, k], at_x(other)).wait_send()
        for d in order:
            z_copy(k, d).wait_send()

        for s in range(n):
            @pl.when(jnp.logical_and(s <= r, r < n - 1))
            def _():
                up_copy(k, s).wait_send()

            @pl.when(jnp.logical_and(s >= r, r > 0))
            def _():
                down_copy(k, s).wait_send()

        return carry

    lax.fori_loop(0, chunks, drain, 0)


def layer(sizes, attn_out, residual, proj_weight, norm_gain, gate_proj, up_proj, down_proj):
    gx, n, gz = sizes
    rows, home = residual.shape
    depth = gate_proj.shape[0]
    hidden = gate_proj.shape[1] // gx
    width = home * n * gz
    chunk = LANES
    chunks = hidden // chunk
    cols = down_proj.shape[1]
    half = home // 2
    lanes = -(-rows // LANES) * LANES
    bf16, f32 = jnp.bfloat16, jnp.float32
    dma, vm = pltpu.SemaphoreType.DMA, pltpu.VMEM
    scratch = [
        vm((2, chunks, 2 * depth, 2 * chunk), bf16),
        vm((max(2 * home, hidden), cols), bf16),
        vm((n, 2, rows, half), bf16),
        vm((2, 2, rows, half), bf16),
        vm((rows, home), bf16),
        vm((rows, home), f32),
        vm((2, rows, half), bf16),
        vm((1, home), f32),
        vm((gx, rows, home), bf16),
        vm((2, rows, half), bf16),
        vm((chunks, n, rows, 2 * chunk), bf16),
        vm((chunks, n, rows, 2 * chunk), bf16),
        vm((chunks, n + 1, rows, 2 * chunk), bf16),
        vm((chunks, n, rows, chunk), bf16),
        vm((n, rows, cols), f32),
        vm((rows, 2 * chunk), f32),
        vm((rows, chunk), f32),
        vm((8, lanes), f32),
        vm((2 * n, 8, lanes), f32),
        vm((2, rows, cols), bf16), vm((2, rows, cols), bf16),
        vm((2, rows, half), bf16), vm((2, rows, half), bf16),
        vm((2, rows, half), bf16), vm((2, rows, half), bf16),
        vm((rows, half), bf16), vm((rows, half), bf16),
        vm((rows, half), bf16), vm((rows, half), bf16),
        dma((2, chunks)), dma((2, chunks)), dma((2, chunks)), dma((chunks,)),
        dma, dma, dma, dma((2,)),
        dma((2,)), dma((n, 2)), dma((n, 2)), dma((n, 2)), dma((n, 2)), dma((2, 2)),
        dma((4, 2)), dma((gx, 2)), dma((2,)), dma((gx, gz)), dma((2 * n,)),
        dma, dma((chunks, n)), dma((chunks, n)), dma((chunks, n + 1)),
        dma((chunks, n)), dma((chunks, n)), dma((chunks, n)), dma((8,)), dma((8,)),
    ]
    away = pl.BlockSpec(memory_space=pl.ANY)
    return pl.pallas_call(
        functools.partial(layer_kernel, n, chunk, width),
        out_shape=jax.ShapeDtypeStruct((rows, home), bf16),
        in_specs=[away] * 7,
        out_specs=pl.BlockSpec(memory_space=pltpu.VMEM),
        scratch_shapes=scratch,
        compiler_params=pltpu.CompilerParams(
            collective_id=0, has_side_effects=True, vmem_limit_bytes=67043328),
    )(attn_out, residual, norm_gain[None, :], proj_weight, gate_proj, up_proj, down_proj)


def on_device(sizes, attn_out, residual, proj_weight, norm_gain, gate_proj, up_proj, down_proj):
    gx, gy, gz = sizes
    assert gx == gy
    if gx == 4 and gz == 2:
        return layer(sizes, attn_out, residual, proj_weight, norm_gain, gate_proj, up_proj, down_proj)
    rows, home = residual.shape
    width = home * gy * gz
    x, z = lax.axis_index("gx"), lax.axis_index("gz")

    turn = [(i * gy + j, j * gy + i) for i in range(gx) for j in range(gy)]
    turned = lax.ppermute(attn_out, ("gx", "gy"), turn)
    cut = turned.shape[1] // 2
    attn_cols = [
        lax.all_gather(turned[:, at:at + cut], "gy", axis=0, tiled=True) for at in (0, cut)
    ]

    def scattered(lefts, weight):
        done, total = 0, None
        for left in lefts:
            depth = left.shape[1]
            part = product(left, lax.slice_in_dim(weight, done, done + depth, axis=0))
            done += depth
            total = part if total is None else total + part

        def columns(zrel):
            def term(xrel):
                at = ((x ^ xrel) * rows, (z ^ zrel) * home)
                return lax.dynamic_slice(total, at, (rows, home))
            return reduced(term, "gx", gx)
        return reduced(columns, "gz", gz)

    projected = scattered(attn_cols, proj_weight)
    stream = residual.astype(jnp.float32) + projected
    scaled = (stream * norm_gain[None, :]).astype(jnp.bfloat16)
    squares = jnp.sum(stream * stream, axis=1)
    scaled = lax.all_gather(scaled, "gz", axis=1, tiled=True)
    scaled = lax.all_to_all(scaled, "gx", split_axis=1, concat_axis=0, tiled=True)
    for axis, size in (("gy", gy), ("gz", gz)):
        bit = 1
        while bit < size:
            squares = squares + swapped(squares, axis, size, bit)
            bit *= 2
    squares = lax.ppermute(squares, ("gx", "gy"), turn)
    inverse = lax.rsqrt(squares / width + 1e-05)[:, None]

    block = gate_proj.shape[1] // gx
    head = 3 * block // 7
    top = gx // 2

    def term_of(weight, at, size, left):
        def term(rel):
            return product(
                left, lax.dynamic_slice_in_dim(weight, (x ^ rel) * block + at, size, 1)
            )
        return term

    def far(at, size, left):
        return [
            halved(term_of(weight, at, size, left), "gx", gx, top, top).astype(jnp.bfloat16)
            for weight in (gate_proj, up_proj)
        ]

    def joined(at, size, left, arrived):
        parts = [
            (halved(term_of(weight, at, size, left), "gx", gx, top) + part.astype(jnp.float32))
            for weight, part in zip((gate_proj, up_proj), arrived)
        ]
        return jnp.concatenate([part.astype(jnp.bfloat16) for part in parts], axis=1)

    def activated(both):
        both = lax.psum_scatter(both, "gy", scatter_dimension=0, tiled=True).astype(jnp.float32)
        half = both.shape[1] // 2
        gate_sum, up_sum = inverse * both[:, :half], inverse * both[:, half:]
        piece = (jax.nn.silu(gate_sum) * up_sum).astype(jnp.bfloat16)
        return lax.all_gather(piece, "gy", axis=0, tiled=True)

    first = [swapped(part, "gx", gx, top) for part in far(0, head, scaled)]
    second = far(head, block - head, scaled)
    first, second = lax.optimization_barrier((first, second))
    second = [swapped(part, "gx", gx, top) for part in second]
    early = activated(joined(0, head, scaled, first))
    late = joined(head, block - head, scaled, second)
    early, late = lax.optimization_barrier((early, late))
    hidden = [early, activated(late)]

    down_sum = scattered(hidden, down_proj)
    return (stream + down_sum).astype(jnp.bfloat16)


def solution(mesh):
    sizes = tuple(mesh.shape[name] for name in ("gx", "gy", "gz"))
    in_specs = (
        P("gx", ("gz", "gy")),
        P("gx", ("gy", "gz")),
        P(("gz", "gx"), "gy"),
        P(("gy", "gz")),
        P(("gy", "gx"), "gz"),
        P(("gy", "gx"), "gz"),
        P(("gz", "gx"), "gy"),
    )
    out_specs = P("gx", ("gy", "gz"))
    return jax.shard_map(
        lambda *args: on_device(sizes, *args),
        mesh=mesh, in_specs=in_specs, out_specs=out_specs, check_vma=False,
    )
```
